32 devices in a mesh: station: 16 (over z, x, core), chan: 2 (over y).
Axes of the slice: x: 2, y: 2, z: 4, core: 2. Of those that a mesh axis runs over, the one named last changes fastest.
Arguments:
- samples: float32 [2, 16, 256, 128, 256], P(None, 'station', 'chan'), may hold values from -6 to 6
- weights: float32 [2, 16, 32, 256, 256], P(None, 'station', None, 'chan'), may hold values from -6 to 6
- antenna_flags: int32 [16, 256], P('station', 'chan'), may hold values from 0 to 1, as said below
- subband_table: int32 [256], replicated, may hold values from 0 to 255, each once
Outputs:
- visibilities: float32 [256, 2, 16, 32, 16], P('chan', None, 'station')
The draws below stay inside these ranges and needn't reach their ends.
Inputs may be any that keep to these rules, and one draw needn't show every extreme that they name: `antenna_flags`: every station has at least 32 antennas with flag 1. `subband_table`: a permutation of 0 to 255.
All inputs are finite; a program needn't handle non-finite values.
Results may differ from the reference program's by a relative error of at most 0.0019.
Values may be sent and summed in bfloat16 or wider, within the bound.
A program may use at most 192 MiB of HBM per device.

```python
import jax
import jax.numpy as jnp
from jax import lax

STATION_ANTENNAS = 256
SUBBAND_COUNT = 256
STATION_BEAMS = 32
TIME_SAMPLES = 128
STATION_COUNT = 16


def draw_antenna_flags(key, part):
    initial_key, second_key = jax.random.split(jax.random.fold_in(key, 11))
    antenna_indices = jnp.arange(STATION_ANTENNAS, dtype=jnp.int32)
    slope_level = 5 + 90 * antenna_indices // STATION_ANTENNAS
    cyclic_shifts = jax.random.randint(initial_key, (STATION_COUNT, STATION_ANTENNAS), 0, 100)
    comb_phase = jax.random.randint(second_key, (STATION_COUNT, 1), 0, 8)
    usable = (cyclic_shifts < slope_level[None, :]) | (antenna_indices[None, :] % 8 == comb_phase)
    return usable.astype(jnp.int32)


def levels(rng, extent, cuts, low, largest):
    loudness, own = 1.0, jax.random.fold_in(rng, 6)
    for position, blocks in cuts:
        heights = jnp.exp(jax.random.uniform(jax.random.fold_in(own, position), (blocks,), jnp.float32, low / len(cuts), largest / len(cuts)))
        loudness = loudness * jnp.repeat(heights, extent[position] // blocks).reshape([-1 if axis == position else 1 for axis in range(len(extent))])
    return loudness


def normal_values(key, dims, scale, bound, cuts=(), held_as=jnp.bfloat16):
    values = scale * jax.random.normal(key, dims, jnp.float32)
    if cuts:
        values = values * levels(key, dims, cuts, -0.22, 0.18)
    return jnp.clip(values, -bound, bound).astype(held_as)


def setup_inputs(seed: int = 0) -> dict:
    arg_keys = jax.random.split(jax.random.key(seed), 5)
    return {
        "samples": normal_values(arg_keys[0], (2, STATION_COUNT, STATION_ANTENNAS, TIME_SAMPLES, SUBBAND_COUNT), 1.0, 6.0, ((1, 16), (2, 2)), jnp.float32),
        "weights": normal_values(arg_keys[1], (2, STATION_COUNT, STATION_BEAMS, STATION_ANTENNAS, SUBBAND_COUNT), 1.0, 6.0, ((1, 16), (3, 2)), jnp.float32),
        "antenna_flags": draw_antenna_flags(jax.random.fold_in(arg_keys[4], 71), 0),
        "subband_table": jax.random.permutation(arg_keys[3], SUBBAND_COUNT).astype(jnp.int32),
    }


def contract_beam(steer, signal):
    return jnp.einsum('baf,atf->fbt', steer, signal, precision=lax.Precision.HIGHEST)

def contract_pair(left, right):
    return jnp.einsum('sfbt,rfbt->fsbr', left, right, precision=lax.Precision.HIGHEST)

def reference(samples, weights, antenna_flags, subband_table):
    usable = antenna_flags.astype(jnp.float32)
    gain_scale = lax.rsqrt(lax.optimization_barrier(jnp.sum(usable, axis=1)))

    def station_beams(packed):
        signal, steer, usable_row = packed
        signal = jnp.take(signal * usable_row[None, :, None, None], subband_table, axis=3)
        steer = jnp.take(steer, subband_table, axis=3)
        real_part = contract_beam(steer[0], signal[0]) - contract_beam(steer[1], signal[1])
        imag_part = contract_beam(steer[0], signal[1]) + contract_beam(steer[1], signal[0])
        return jnp.stack([real_part, imag_part], axis=1)
    beam_sum = lax.map(station_beams, (jnp.moveaxis(samples, 1, 0), jnp.moveaxis(weights, 1, 0), usable))
    beam_data = (beam_sum * gain_scale[:, None, None, None, None]).astype(jnp.bfloat16)
    signal = beam_data.astype(jnp.float32)
    real_part = contract_pair(signal[:, :, 0], signal[:, :, 0]) + contract_pair(signal[:, :, 1], signal[:, :, 1])
    imag_part = contract_pair(signal[:, :, 1], signal[:, :, 0]) - contract_pair(signal[:, :, 0], signal[:, :, 1])
    return jnp.stack([real_part, imag_part], axis=1)
```

```python
import functools

import jax
import jax.numpy as jnp
from jax import lax
from jax.experimental import pallas as pl
from jax.experimental.pallas import tpu as pltpu
from jax.sharding import PartitionSpec as P

LANES = 128
SLAB = 64
SLABS_PER_CHUNK = 8
CHUNKS_IN_FLIGHT = 8
GROUP = 4
TILE_BEAMS = 16


def split(value):
    high = value.astype(jnp.bfloat16)
    low = (value - high.astype(jnp.float32)).astype(jnp.bfloat16)
    return high, low


def kernel(
    table_ref, flags_ref, x_hbm, w_hbm, out_ref,
    x_rows, w_rows, chunk_buf, own, partials, arrived, gathered, results, returned, count_ref, counts,
    chunk_sem, count_send, count_recv, chan_send, chan_recv, beam_send, beam_recv, back_send, back_recv,
):
    groups, stations = lax.axis_size("chan"), lax.axis_size("station")
    mine, me = lax.axis_index("chan"), lax.axis_index("station")
    halves, share = gathered.shape[0], gathered.shape[1]
    antennas = x_hbm.shape[2]
    subbands = x_hbm.shape[4]
    beams = gathered.shape[3]
    kept = subbands // groups
    blocks = subbands // LANES
    tall = min(antennas, SLAB)
    x_stride = x_rows.shape[2]
    w_stride = w_rows.shape[1]
    w_chunks = w_hbm.shape[2] // SLABS_PER_CHUNK
    x_chunks = antennas // SLABS_PER_CHUNK
    chunks = w_chunks + halves * x_chunks
    beams_per_chunk = SLABS_PER_CHUNK * SLAB // antennas
    parts_of_phase = stations // GROUP
    x_lines = x_rows.reshape(halves, subbands * x_stride, LANES)
    w_lines = w_rows.reshape(subbands * w_stride, LANES)

    def target(k):
        return lax.rem(me + stations // 2 + ((k + 1) // 2) * (1 - 2 * lax.rem(k, 2)), stations)

    def remote(src, dst, send, recv, device):
        return pltpu.make_async_remote_copy(
            src_ref=src, dst_ref=dst, send_sem=send, recv_sem=recv,
            device_id=device, device_id_type=pl.DeviceIdType.MESH,
        )

    def chan_copy(g, h, i, q):
        peer = lax.rem(mine + g, groups)
        return remote(
            partials.at[g - 1, h, i, q], arrived.at[g - 1, h, i, q],
            chan_send.at[g - 1, h, i, q], chan_recv.at[g - 1, h, i, q], (me, peer),
        )

    def count_copy(g):
        return remote(
            count_ref, counts.at[g - 1], count_send.at[g - 1], count_recv.at[g - 1], (me, lax.rem(mine + g, groups))
        )

    def beam_copy(h, i, q, u):
        k = q * GROUP + u
        return remote(
            arrived.at[0, h, i, q, u], gathered.at[h, i, me],
            beam_send.at[h, i, k], beam_recv.at[h, i, k], (target(k), mine),
        )

    def back_copy(i, k):
        there = target(k)
        return remote(
            results.at[i, there], returned.at[i * stations + me],
            back_send.at[i, k], back_recv.at[i, k], (there, mine),
        )

    def w_copy(n, slot):
        return pltpu.make_async_copy(
            w_hbm.at[:, 0, pl.ds(n * SLABS_PER_CHUNK, SLABS_PER_CHUNK)], chunk_buf.at[slot], chunk_sem.at[slot]
        )

    def x_copy(n, slot):
        half = n // x_chunks
        first = lax.rem(n, x_chunks) * SLABS_PER_CHUNK
        return pltpu.make_async_copy(
            x_hbm.at[:, 0, pl.ds(first, SLABS_PER_CHUNK), pl.ds(half * SLAB, SLAB)],
            chunk_buf.at[slot], chunk_sem.at[slot],
        )

    def slot_of(n):
        return lax.rem(n, CHUNKS_IN_FLIGHT)

    def start_chunk(n):
        @pl.when(n < w_chunks)
        def _():
            w_copy(n, slot_of(n)).start()

        @pl.when((n >= w_chunks) & (n < chunks))
        def _():
            x_copy(n - w_chunks, slot_of(n)).start()

    for n in range(min(CHUNKS_IN_FLIGHT, chunks)):
        if n < w_chunks:
            w_copy(n, n % CHUNKS_IN_FLIGHT).start()
        else:
            x_copy(n - w_chunks, n % CHUNKS_IN_FLIGHT).start()

    barrier = pltpu.get_barrier_semaphore()
    for g in range(1, groups):
        pl.semaphore_signal(
            barrier, inc=1, device_id=(me, lax.rem(mine + g, groups)), device_id_type=pl.DeviceIdType.MESH
        )

    @pl.loop(0, stations - 1)
    def _(k):
        pl.semaphore_signal(barrier, inc=1, device_id=(target(k), mine), device_id_type=pl.DeviceIdType.MESH)

    usable = flags_ref[...].astype(jnp.float32)
    count_ref[...] = jnp.broadcast_to(jnp.sum(usable, axis=1, keepdims=True), count_ref.shape)
    if antennas < LANES:
        usable = jnp.concatenate([usable, jnp.zeros((1, LANES - antennas), jnp.float32)], axis=1)

    @pl.loop(0, w_chunks)
    def _(n):
        slot = slot_of(n)
        w_copy(n, slot).wait()
        for part in range(2):
            for b in range(beams_per_chunk):
                for block in range(blocks):
                    lanes = slice(block * LANES, (block + 1) * LANES)
                    tiles = [
                        chunk_buf[slot, part, row // SLAB, row % SLAB : row % SLAB + tall, lanes]
                        for row in range(b * antennas, (b + 1) * antennas, tall)
                    ]
                    if antennas < LANES:
                        tiles.append(jnp.zeros((LANES - antennas, LANES), jnp.float32))
                    row = block * LANES * w_stride + part * beams + n * beams_per_chunk + b
                    w_lines[pl.ds(row, LANES, stride=w_stride), :] = jnp.concatenate(tiles, axis=0).T * usable
        start_chunk(n + CHUNKS_IN_FLIGHT)

    def turn(h, first, last):
        @pl.loop(first, last)
        def _(m):
            n = w_chunks + h * x_chunks + m
            slot = slot_of(n)
            x_copy(h * x_chunks + m, slot).wait()
            for a in range(SLABS_PER_CHUNK):
                for block in range(blocks):
                    lanes = pl.ds(block * LANES, LANES)
                    tile = jnp.concatenate([chunk_buf[slot, part, a, :, lanes] for part in range(2)], axis=0)
                    row = block * LANES * x_stride + m * SLABS_PER_CHUNK + a
                    x_lines[h, pl.ds(row, LANES, stride=x_stride), :] = tile.T
            start_chunk(n + CHUNKS_IN_FLIGHT)

    turn(0, 0, x_chunks)

    pl.semaphore_wait(barrier, groups - 1 + stations - 1)
    for g in range(1, groups):
        count_copy(g).start()

    lane = lax.broadcasted_iota(jnp.int32, (beams, LANES), 1)
    sign = jnp.where(lane < SLAB, -1.0, 1.0).astype(jnp.float32)

    def partial(h, slot):
        f = table_ref[slot]
        x = x_rows[h, f, :antennas, :]
        w = w_rows[f, : 2 * beams, :antennas]
        x_pair = jnp.concatenate(split(x), axis=0)
        w_high, w_low = split(w)
        grid = jnp.dot(
            jnp.concatenate([w_high, w_high], axis=1), x_pair, preferred_element_type=jnp.float32
        ) + jnp.dot(jnp.concatenate([w_low, w_low], axis=1), x_pair, preferred_element_type=jnp.float32)
        return grid[:beams] + pltpu.roll(grid[beams:], SLAB, axis=1) * sign

    def peers(h, i):
        for g in range(1, groups):
            first = lax.rem(mine + g, groups) * kept + i * stations

            @pl.loop(0, parts_of_phase)
            def _(q):
                for u in range(GROUP):
                    total = partial(h, first + target(q * GROUP + u))
                    partials[g - 1, h, i, q, u] = total.astype(jnp.bfloat16)
                chan_copy(g, h, i, q).start()

    def own_sums(h, i):
        first = mine * kept + i * stations

        @pl.loop(0, parts_of_phase)
        def _(q):
            for u in range(GROUP):
                own[q, u] = partial(h, first + target(q * GROUP + u))

    def forward(h, i, gain):
        def piece(q, last):
            for g in range(1, groups):
                chan_copy(g, h, i, q).wait_recv()
            for u in range(GROUP):
                total = own[q, u]
                for g in range(1, groups):
                    total = total + arrived[g - 1, h, i, q, u].astype(jnp.float32)
                value = (total * gain).astype(jnp.bfloat16)
                if last and u == GROUP - 1:
                    gathered[h, i, me] = value
                else:
                    arrived[0, h, i, q, u] = value
                    beam_copy(h, i, q, u).start()

        @pl.loop(0, parts_of_phase - 1)
        def _(q):
            piece(q, False)

        piece(parts_of_phase - 1, True)

    tile_rows = stations * TILE_BEAMS
    mask = lax.broadcasted_iota(jnp.int32, (TILE_BEAMS, tile_rows), 0) == lax.rem(
        lax.broadcasted_iota(jnp.int32, (TILE_BEAMS, tile_rows), 1), TILE_BEAMS
    )
    chosen = mask.astype(jnp.float32).reshape(1, TILE_BEAMS, tile_rows)
    wide = tile_rows // LANES
    beam_tiles = beams // TILE_BEAMS
    result_rows = 2 * beam_tiles * wide

    def correlate(i):
        for h in range(halves):
            @pl.loop(0, stations - 1)
            def _(k):
                beam_copy(h, i, k // GROUP, lax.rem(k, GROUP)).wait_recv()

        for tile in range(beam_tiles):
            straight, turned = [], []
            for h in range(halves):
                y = gathered[h, i, :, pl.ds(tile * TILE_BEAMS, TILE_BEAMS), :].reshape(tile_rows, LANES)
                straight.append(y)
                swapped = jnp.concatenate([y[:, SLAB:], -y[:, :SLAB]], axis=1)
                turned.append(swapped)
            y = jnp.concatenate(straight, axis=1)
            for part, x in enumerate((y, jnp.concatenate(turned, axis=1))):
                pairs = lax.dot_general(x, y, (((1,), (1,)), ((), ())), preferred_element_type=jnp.float32)
                total = jnp.sum(pairs.reshape(stations, TILE_BEAMS, tile_rows) * chosen, axis=1)
                for piece in range(wide):
                    row = (part * beam_tiles + tile) * wide + piece
                    results[i, :, row, :] = total[:, piece * LANES : (piece + 1) * LANES]

        @pl.loop(0, stations - 1)
        def _(k):
            back_copy(i, k).start()

        returned[i * stations + me] = results[i, me]

    peers(0, 0)
    count = count_ref[...]
    for g in range(1, groups):
        count_copy(g).wait_recv()
        count = count + counts[g - 1]
    gain = lax.rsqrt(count)[0:1, :]

    each = x_chunks // share
    for h in range(halves):
        @pl.loop(0, share)
        def _(i):
            own_sums(h, i)
            if h + 1 < halves:
                turn(h + 1, i * each, (i + 1) * each)

            @pl.when(i + 1 < share)
            def _():
                peers(h, i + 1)

            if h + 1 < halves:
                @pl.when(i + 1 == share)
                def _():
                    peers(h + 1, 0)

            forward(h, i, gain)
            if h + 1 == halves:
                @pl.when(i > 0)
                def _():
                    correlate(i - 1)

    correlate(share - 1)

    @pl.loop(0, share)
    def _(i):
        @pl.loop(0, stations - 1)
        def _(k):
            back_copy(i, k).wait_recv()

    per_row = LANES // TILE_BEAMS
    for part in range(2):
        for tile in range(beam_tiles):
            for piece in range(wide):
                row = (part * beam_tiles + tile) * wide + piece
                turned = returned[:, row, :].T
                for r in range(per_row):
                    out_ref[part, pl.ds(tile * TILE_BEAMS, TILE_BEAMS), piece * per_row + r, :] = turned[
                        r * TILE_BEAMS : (r + 1) * TILE_BEAMS
                    ]

    for g in range(1, groups):
        count_copy(g).wait_send()
    for h in range(halves):
        @pl.loop(0, share)
        def _(i):
            @pl.loop(0, parts_of_phase)
            def _(q):
                for g in range(1, groups):
                    chan_copy(g, h, i, q).wait_send()

            @pl.loop(0, stations - 1)
            def _(k):
                beam_copy(h, i, k // GROUP, lax.rem(k, GROUP)).wait_send()

    @pl.loop(0, share)
    def _(i):
        @pl.loop(0, stations - 1)
        def _(k):
            back_copy(i, k).wait_send()


def on_device(samples, weights, antenna_flags, subband_table):
    groups, stations = lax.axis_size("chan"), lax.axis_size("station")
    _, _, antennas, times, subbands = samples.shape
    beams = weights.shape[2]
    kept = subbands // groups
    share = kept // stations
    halves = times // SLAB
    quarters = stations // GROUP
    rows = 2 * (beams // TILE_BEAMS) * (stations * TILE_BEAMS // LANES)
    slabs = weights.reshape(2, 1, beams * antennas // SLAB, SLAB, subbands)
    dma = pltpu.SemaphoreType.DMA
    out = pl.pallas_call(
        kernel,
        out_shape=jax.ShapeDtypeStruct((2, beams, stations, kept), jnp.float32),
        in_specs=[
            pl.BlockSpec(memory_space=pltpu.SMEM),
            pl.BlockSpec(memory_space=pltpu.VMEM),
            pl.BlockSpec(memory_space=pl.ANY),
            pl.BlockSpec(memory_space=pl.ANY),
        ],
        out_specs=pl.BlockSpec(memory_space=pltpu.VMEM),
        scratch_shapes=[
            pltpu.VMEM((halves, subbands, antennas + 8, LANES), jnp.float32),
            pltpu.VMEM((subbands, 2 * beams + 8, LANES), jnp.float32),
            pltpu.VMEM((CHUNKS_IN_FLIGHT, 2, SLABS_PER_CHUNK, SLAB, subbands), jnp.float32),
            pltpu.VMEM((quarters, GROUP, beams, LANES), jnp.float32),
            pltpu.VMEM((groups - 1, halves, share, quarters, GROUP, beams, LANES), jnp.bfloat16),
            pltpu.VMEM((groups - 1, halves, share, quarters, GROUP, beams, LANES), jnp.bfloat16),
            pltpu.VMEM((halves, share, stations, beams, LANES), jnp.bfloat16),
            pltpu.VMEM((share, stations, rows, LANES), jnp.float32),
            pltpu.VMEM((kept, rows, LANES), jnp.float32),
            pltpu.VMEM((8, LANES), jnp.float32),
            pltpu.VMEM((groups - 1, 8, LANES), jnp.float32),
            dma((CHUNKS_IN_FLIGHT,)),
            dma((groups - 1,)),
            dma((groups - 1,)),
            dma((groups - 1, halves, share, quarters)),
            dma((groups - 1, halves, share, quarters)),
            dma((halves, share, stations)),
            dma((halves, share, stations)),
            dma((share, stations)),
            dma((share, stations)),
        ],
        compiler_params=pltpu.CompilerParams(
            collective_id=0, has_side_effects=True, vmem_limit_bytes=67043328
        ),
    )(subband_table, antenna_flags, samples, slabs)
    return out.transpose(3, 0, 1, 2)[:, :, None]


def solution(mesh):
    in_specs = (
        P(None, "station", "chan", None, None),
        P(None, "station", None, "chan", None),
        P("station", "chan"),
        P(),
    )
    out_specs = P("chan", None, "station", None, None)
    return jax.shard_map(
        on_device, mesh=mesh, in_specs=in_specs, out_specs=out_specs, check_vma=False
    )
```

```python
import functools

import jax
import jax.numpy as jnp
from jax import lax
from jax.experimental import pallas as pl
from jax.experimental.pallas import tpu as pltpu
from jax.sharding import PartitionSpec as P

LANES = 128
SLAB = 64
SLABS_PER_CHUNK = 8
CHUNKS_IN_FLIGHT = 8
GROUP = 8
TILE_BEAMS = 16


def split(value):
    high = value.astype(jnp.bfloat16)
    low = (value - high.astype(jnp.float32)).astype(jnp.bfloat16)
    return high, low


def kernel(
    table_ref, flags_ref, x_hbm, w_hbm, out_ref,
    x_rows, w_rows, chunk_buf, own, partials, arrived, gathered, results, returned, count_ref, counts,
    chunk_sem, count_send, count_recv, chan_send, chan_recv, beam_send, beam_recv, back_send, back_recv,
):
    groups, stations = lax.axis_size("chan"), lax.axis_size("station")
    mine, me = lax.axis_index("chan"), lax.axis_index("station")
    halves, share = gathered.shape[0], gathered.shape[1]
    antennas = x_hbm.shape[2]
    subbands = x_hbm.shape[4]
    beams = gathered.shape[3]
    kept = subbands // groups
    blocks = subbands // LANES
    tall = min(antennas, SLAB)
    x_stride = x_rows.shape[2]
    w_stride = w_rows.shape[1]
    w_chunks = w_hbm.shape[2] // SLABS_PER_CHUNK
    x_chunks = antennas // SLABS_PER_CHUNK
    chunks = w_chunks + halves * x_chunks
    beams_per_chunk = SLABS_PER_CHUNK * SLAB // antennas
    parts_of_phase = stations // GROUP
    x_lines = x_rows.reshape(halves, subbands * x_stride, LANES)
    w_lines = w_rows.reshape(subbands * w_stride, LANES)

    def target(k):
        return lax.rem(me + stations // 2 + ((k + 1) // 2) * (1 - 2 * lax.rem(k, 2)), stations)

    def remote(src, dst, send, recv, device):
        return pltpu.make_async_remote_copy(
            src_ref=src, dst_ref=dst, send_sem=send, recv_sem=recv,
            device_id=device, device_id_type=pl.DeviceIdType.MESH,
        )

    def chan_copy(g, h, i, q):
        peer = lax.rem(mine + g, groups)
        return remote(
            partials.at[g - 1, h, i, q], arrived.at[g - 1, h, i, q],
            chan_send, chan_recv.at[g - 1, h, i, q], (me, peer),
        )

    def count_copy(g):
        return remote(
            count_ref, counts.at[g - 1], count_send.at[g - 1], count_recv.at[g - 1], (me, lax.rem(mine + g, groups))
        )

    def beam_copy(h, i, q, u):
        return remote(
            arrived.at[0, h, i, q, u], gathered.at[h, i, me],
            beam_send, beam_recv.at[i], (target(q * GROUP + u), mine),
        )

    def back_copy(i, k):
        there = target(k)
        return remote(
            results.at[i, there], returned.at[i * stations + me],
            back_send, back_recv, (there, mine),
        )

    def all_of(ref, send, recv):
        return remote(ref, ref, send, recv, (me, lax.rem(mine + 1, groups)))

    others = pl.ds(0, stations - 1)

    def w_copy(n, slot):
        return pltpu.make_async_copy(
            w_hbm.at[:, 0, pl.ds(n * SLABS_PER_CHUNK, SLABS_PER_CHUNK)], chunk_buf.at[slot], chunk_sem.at[slot]
        )

    def x_copy(n, slot):
        half = n // x_chunks
        first = lax.rem(n, x_chunks) * SLABS_PER_CHUNK
        return pltpu.make_async_copy(
            x_hbm.at[:, 0, pl.ds(first, SLABS_PER_CHUNK), pl.ds(half * SLAB, SLAB)],
            chunk_buf.at[slot], chunk_sem.at[slot],
        )

    def slot_of(n):
        return lax.rem(n, CHUNKS_IN_FLIGHT)

    def start_chunk(n):
        @pl.when(n < w_chunks)
        def _():
            w_copy(n, slot_of(n)).start()

        @pl.when((n >= w_chunks) & (n < chunks))
        def _():
            x_copy(n - w_chunks, slot_of(n)).start()

    for n in range(min(CHUNKS_IN_FLIGHT, chunks)):
        if n < w_chunks:
            w_copy(n, n % CHUNKS_IN_FLIGHT).start()
        else:
            x_copy(n - w_chunks, n % CHUNKS_IN_FLIGHT).start()

    barrier = pltpu.get_barrier_semaphore()
    for g in range(1, groups):
        pl.semaphore_signal(
            barrier, inc=1, device_id=(me, lax.rem(mine + g, groups)), device_id_type=pl.DeviceIdType.MESH
        )

    @pl.loop(0, stations - 1)
    def _(k):
        pl.semaphore_signal(barrier, inc=1, device_id=(target(k), mine), device_id_type=pl.DeviceIdType.MESH)

    usable = flags_ref[...].astype(jnp.float32)
    count_ref[...] = jnp.broadcast_to(jnp.sum(usable, axis=1, keepdims=True), count_ref.shape)
    if antennas < LANES:
        usable = jnp.concatenate([usable, jnp.zeros((1, LANES - antennas), jnp.float32)], axis=1)

    @pl.loop(0, w_chunks)
    def _(n):
        slot = slot_of(n)
        w_copy(n, slot).wait()
        for part in range(2):
            for b in range(beams_per_chunk):
                for block in range(blocks):
                    lanes = slice(block * LANES, (block + 1) * LANES)
                    tiles = [
                        chunk_buf[slot, part, row // SLAB, row % SLAB : row % SLAB + tall, lanes]
                        for row in range(b * antennas, (b + 1) * antennas, tall)
                    ]
                    if antennas < LANES:
                        tiles.append(jnp.zeros((LANES - antennas, LANES), jnp.float32))
                    row = block * LANES * w_stride + part * beams + n * beams_per_chunk + b
                    w_lines[pl.ds(row, LANES, stride=w_stride), :] = jnp.concatenate(tiles, axis=0).T * usable
        start_chunk(n + CHUNKS_IN_FLIGHT)

    def turn(h, first, last):
        @pl.loop(first, last)
        def _(m):
            n = w_chunks + h * x_chunks + m
            slot = slot_of(n)
            x_copy(h * x_chunks + m, slot).wait()
            for a in range(SLABS_PER_CHUNK):
                for block in range(blocks):
                    lanes = pl.ds(block * LANES, LANES)
                    tile = jnp.concatenate([chunk_buf[slot, part, a, :, lanes] for part in range(2)], axis=0)
                    row = block * LANES * x_stride + m * SLABS_PER_CHUNK + a
                    x_lines[h, pl.ds(row, LANES, stride=x_stride), :] = tile.T
            start_chunk(n + CHUNKS_IN_FLIGHT)

    turn(0, 0, x_chunks)

    pl.semaphore_wait(barrier, groups - 1 + stations - 1)
    for g in range(1, groups):
        count_copy(g).start()

    lane = lax.broadcasted_iota(jnp.int32, (beams, LANES), 1)
    sign = jnp.where(lane < SLAB, -1.0, 1.0).astype(jnp.float32)

    def partial(h, slot):
        f = table_ref[slot]
        x = x_rows[h, f, :antennas, :]
        w = w_rows[f, : 2 * beams, :antennas]
        x_pair = jnp.concatenate(split(x), axis=0)
        w_high, w_low = split(w)
        grid = jnp.dot(
            jnp.concatenate([w_high, w_high], axis=1), x_pair, preferred_element_type=jnp.float32
        ) + jnp.dot(jnp.concatenate([w_low, w_low], axis=1), x_pair, preferred_element_type=jnp.float32)
        return grid[:beams] + pltpu.roll(grid[beams:], SLAB, axis=1) * sign

    def peers(h, i):
        for g in range(1, groups):
            first = lax.rem(mine + g, groups) * kept + i * stations

            @pl.loop(0, parts_of_phase)
            def _(q):
                for u in range(GROUP):
                    total = partial(h, first + target(q * GROUP + u))
                    partials[g - 1, h, i, q, u] = total.astype(jnp.bfloat16)
                chan_copy(g, h, i, q).start()

    def own_sums(h, i):
        first = mine * kept + i * stations

        @pl.loop(0, parts_of_phase)
        def _(q):
            for u in range(GROUP):
                own[q, u] = partial(h, first + target(q * GROUP + u))

    def forward(h, i, gain):
        def piece(q, last):
            for g in range(1, groups):
                chan_copy(g, h, i, q).wait_recv()
            for u in range(GROUP):
                total = own[q, u]
                for g in range(1, groups):
                    total = total + arrived[g - 1, h, i, q, u].astype(jnp.float32)
                value = (total * gain).astype(jnp.bfloat16)
                if last and u == GROUP - 1:
                    gathered[h, i, me] = value
                else:
                    arrived[0, h, i, q, u] = value
                    beam_copy(h, i, q, u).start()

        @pl.loop(0, parts_of_phase - 1)
        def _(q):
            piece(q, False)

        piece(parts_of_phase - 1, True)

    tile_rows = stations * TILE_BEAMS
    mask = lax.broadcasted_iota(jnp.int32, (TILE_BEAMS, tile_rows), 0) == lax.rem(
        lax.broadcasted_iota(jnp.int32, (TILE_BEAMS, tile_rows), 1), TILE_BEAMS
    )
    chosen = mask.astype(jnp.float32).reshape(1, TILE_BEAMS, tile_rows)
    wide = tile_rows // LANES
    beam_tiles = beams // TILE_BEAMS
    result_rows = 2 * beam_tiles * wide

    def correlate(i):
        all_of(gathered.at[:, i, others], beam_send, beam_recv.at[i]).wait_recv()
        for tile in range(beam_tiles):
            straight, turned = [], []
            for h in range(halves):
                y = gathered[h, i, :, pl.ds(tile * TILE_BEAMS, TILE_BEAMS), :].reshape(tile_rows, LANES)
                straight.append(y)
                swapped = jnp.concatenate([y[:, SLAB:], -y[:, :SLAB]], axis=1)
                turned.append(swapped)
            y = jnp.concatenate(straight, axis=1)
            for part, x in enumerate((y, jnp.concatenate(turned, axis=1))):
                pairs = lax.dot_general(x, y, (((1,), (1,)), ((), ())), preferred_element_type=jnp.float32)
                total = jnp.sum(pairs.reshape(stations, TILE_BEAMS, tile_rows) * chosen, axis=1)
                for piece in range(wide):
                    row = (part * beam_tiles + tile) * wide + piece
                    results[i, :, row, :] = total[:, piece * LANES : (piece + 1) * LANES]

        @pl.loop(0, stations - 1)
        def _(k):
            back_copy(i, k).start()

        returned[i * stations + me] = results[i, me]

    peers(0, 0)
    count = count_ref[...]
    for g in range(1, groups):
        count_copy(g).wait_recv()
        count = count + counts[g - 1]
    gain = lax.rsqrt(count)[0:1, :]

    each = x_chunks // share
    for h in range(halves):
        @pl.loop(0, share)
        def _(i):
            own_sums(h, i)
            if h + 1 < halves:
                turn(h + 1, i * each, (i + 1) * each)

            @pl.when(i + 1 < share)
            def _():
                peers(h, i + 1)

            if h + 1 < halves:
                @pl.when(i + 1 == share)
                def _():
                    peers(h + 1, 0)

            forward(h, i, gain)
            if h + 1 == halves:
                @pl.when(i > 0)
                def _():
                    correlate(i - 1)

    correlate(share - 1)

    all_of(returned.at[pl.ds(0, share * (stations - 1))], back_send, back_recv).wait_recv()

    per_row = LANES // TILE_BEAMS
    for part in range(2):
        for tile in range(beam_tiles):
            for piece in range(wide):
                row = (part * beam_tiles + tile) * wide + piece
                turned = returned[:, row, :].T
                for r in range(per_row):
                    out_ref[part, pl.ds(tile * TILE_BEAMS, TILE_BEAMS), piece * per_row + r, :] = turned[
                        r * TILE_BEAMS : (r + 1) * TILE_BEAMS
                    ]

    for g in range(1, groups):
        count_copy(g).wait_send()
    all_of(partials, chan_send, chan_recv.at[0, 0, 0, 0]).wait_send()
    all_of(gathered.at[:, :, others], beam_send, beam_recv.at[0]).wait_send()
    all_of(results.at[:, others], back_send, back_recv).wait_send()


def on_device(samples, weights, antenna_flags, subband_table):
    groups, stations = lax.axis_size("chan"), lax.axis_size("station")
    _, _, antennas, times, subbands = samples.shape
    beams = weights.shape[2]
    kept = subbands // groups
    share = kept // stations
    halves = times // SLAB
    quarters = stations // GROUP
    rows = 2 * (beams // TILE_BEAMS) * (stations * TILE_BEAMS // LANES)
    slabs = weights.reshape(2, 1, beams * antennas // SLAB, SLAB, subbands)
    dma = pltpu.SemaphoreType.DMA
    out = pl.pallas_call(
        kernel,
        out_shape=jax.ShapeDtypeStruct((2, beams, stations, kept), jnp.float32),
        in_specs=[
            pl.BlockSpec(memory_space=pltpu.SMEM),
            pl.BlockSpec(memory_space=pltpu.VMEM),
            pl.BlockSpec(memory_space=pl.ANY),
            pl.BlockSpec(memory_space=pl.ANY),
        ],
        out_specs=pl.BlockSpec(memory_space=pltpu.VMEM),
        scratch_shapes=[
            pltpu.VMEM((halves, subbands, antennas + 8, LANES), jnp.float32),
            pltpu.VMEM((subbands, 2 * beams + 8, LANES), jnp.float32),
            pltpu.VMEM((CHUNKS_IN_FLIGHT, 2, SLABS_PER_CHUNK, SLAB, subbands), jnp.float32),
            pltpu.VMEM((quarters, GROUP, beams, LANES), jnp.float32),
            pltpu.VMEM((groups - 1, halves, share, quarters, GROUP, beams, LANES), jnp.bfloat16),
            pltpu.VMEM((groups - 1, halves, share, quarters, GROUP, beams, LANES), jnp.bfloat16),
            pltpu.VMEM((halves, share, stations, beams, LANES), jnp.bfloat16),
            pltpu.VMEM((share, stations, rows, LANES), jnp.float32),
            pltpu.VMEM((kept, rows, LANES), jnp.float32),
            pltpu.VMEM((8, LANES), jnp.float32),
            pltpu.VMEM((groups - 1, 8, LANES), jnp.float32),
            dma((CHUNKS_IN_FLIGHT,)),
            dma((groups - 1,)),
            dma((groups - 1,)),
            dma,
            dma((groups - 1, halves, share, quarters)),
            dma,
            dma((share,)),
            dma,
            dma,
        ],
        compiler_params=pltpu.CompilerParams(
            collective_id=0, has_side_effects=True, vmem_limit_bytes=67043328
        ),
    )(subband_table, antenna_flags, samples, slabs)
    return out.transpose(3, 0, 1, 2)[:, :, None]


def solution(mesh):
    in_specs = (
        P(None, "station", "chan", None, None),
        P(None, "station", None, "chan", None),
        P("station", "chan"),
        P(),
    )
    out_specs = P("chan", None, "station", None, None)
    return jax.shard_map(
        on_device, mesh=mesh, in_specs=in_specs, out_specs=out_specs, check_vma=False
    )
```

```python
import functools

import jax
import jax.numpy as jnp
from jax import lax
from jax.experimental import pallas as pl
from jax.experimental.pallas import tpu as pltpu
from jax.sharding import PartitionSpec as P

LANES = 128
SLAB = 64
SLABS_PER_CHUNK = 8
CHUNKS_IN_FLIGHT = 8
GROUP = 8
TILE_BEAMS = 16
AHEAD = 3
BEHIND = 3


def split(value):
    high = value.astype(jnp.bfloat16)
    low = (value - high.astype(jnp.float32)).astype(jnp.bfloat16)
    return high, low


def kernel(
    table_ref, flags_ref, x_hbm, w_hbm, out_ref,
    x_rows, w_rows, chunk_buf, own, partials, arrived, gathered, results, far_results, returned, far_returned, count_ref, counts,
    chunk_sem, count_send, count_recv, chan_send, chan_recv, beam_send, beam_recv, back_send, back_recv,
    far_send, far_recv,
):
    groups, stations = lax.axis_size("chan"), lax.axis_size("station")
    mine, me = lax.axis_index("chan"), lax.axis_index("station")
    halves, share = gathered.shape[0], gathered.shape[1]
    antennas = x_hbm.shape[2]
    subbands = x_hbm.shape[4]
    beams = gathered.shape[3]
    kept = subbands // groups
    blocks = subbands // LANES
    tall = min(antennas, SLAB)
    x_stride = x_rows.shape[2]
    w_stride = w_rows.shape[1]
    w_chunks = w_hbm.shape[2] // SLABS_PER_CHUNK
    x_chunks = antennas // SLABS_PER_CHUNK
    chunks = w_chunks + halves * x_chunks
    beams_per_chunk = SLABS_PER_CHUNK * SLAB // antennas
    parts_of_phase = stations // GROUP
    x_lines = x_rows.reshape(halves, subbands * x_stride, LANES)
    w_lines = w_rows.reshape(subbands * w_stride, LANES)

    def target(k):
        return lax.rem(me + stations // 2 + ((k + 1) // 2) * (1 - 2 * lax.rem(k, 2)), stations)

    def remote(src, dst, send, recv, device):
        return pltpu.make_async_remote_copy(
            src_ref=src, dst_ref=dst, send_sem=send, recv_sem=recv,
            device_id=device, device_id_type=pl.DeviceIdType.MESH,
        )

    def chan_copy(g, h, i, q):
        peer = lax.rem(mine + g, groups)
        return remote(
            partials.at[g - 1, h, i, q], arrived.at[g - 1, h, i, q],
            chan_send, chan_recv.at[g - 1, h, i, q], (me, peer),
        )

    def count_copy(g):
        return remote(
            count_ref, counts.at[g - 1], count_send.at[g - 1], count_recv.at[g - 1], (me, lax.rem(mine + g, groups))
        )

    def beam_copy(h, i, q, u):
        return remote(
            arrived.at[0, h, i, q, u], gathered.at[h, i, me],
            beam_send, beam_recv.at[i], (target(q * GROUP + u), mine),
        )

    half = stations // 2
    near_first = me // half * half
    far_first = half - near_first

    def back_copy(i, k):
        there = near_first + lax.rem(me + 1 + k, half)
        return remote(
            results.at[i, there], returned.at[i * stations + me], back_send, back_recv, (there, mine)
        )

    def far_copy(i, k):
        return remote(
            far_results.at[i, k], far_returned.at[i, lax.rem(me, half)], far_send, far_recv,
            (far_first + k, mine),
        )

    def all_of(ref, send, recv):
        return remote(ref, ref, send, recv, (me, lax.rem(mine + 1, groups)))

    others = pl.ds(0, stations - 1)

    def w_copy(n, slot):
        return pltpu.make_async_copy(
            w_hbm.at[:, 0, pl.ds(n * SLABS_PER_CHUNK, SLABS_PER_CHUNK)], chunk_buf.at[slot], chunk_sem.at[slot]
        )

    def x_copy(n, slot):
        half = n // x_chunks
        first = lax.rem(n, x_chunks) * SLABS_PER_CHUNK
        return pltpu.make_async_copy(
            x_hbm.at[:, 0, pl.ds(first, SLABS_PER_CHUNK), pl.ds(half * SLAB, SLAB)],
            chunk_buf.at[slot], chunk_sem.at[slot],
        )

    def slot_of(n):
        return lax.rem(n, CHUNKS_IN_FLIGHT)

    def start_chunk(n):
        @pl.when(n < w_chunks)
        def _():
            w_copy(n, slot_of(n)).start()

        @pl.when((n >= w_chunks) & (n < chunks))
        def _():
            x_copy(n - w_chunks, slot_of(n)).start()

    for n in range(min(CHUNKS_IN_FLIGHT, chunks)):
        if n < w_chunks:
            w_copy(n, n % CHUNKS_IN_FLIGHT).start()
        else:
            x_copy(n - w_chunks, n % CHUNKS_IN_FLIGHT).start()

    barrier = pltpu.get_barrier_semaphore()
    for g in range(1, groups):
        pl.semaphore_signal(
            barrier, inc=1, device_id=(me, lax.rem(mine + g, groups)), device_id_type=pl.DeviceIdType.MESH
        )

    @pl.loop(0, stations - 1)
    def _(k):
        pl.semaphore_signal(barrier, inc=1, device_id=(target(k), mine), device_id_type=pl.DeviceIdType.MESH)

    usable = flags_ref[...].astype(jnp.float32)
    count_ref[...] = jnp.broadcast_to(jnp.sum(usable, axis=1, keepdims=True), count_ref.shape)
    if antennas < LANES:
        usable = jnp.concatenate([usable, jnp.zeros((1, LANES - antennas), jnp.float32)], axis=1)

    @pl.loop(0, w_chunks)
    def _(n):
        slot = slot_of(n)
        w_copy(n, slot).wait()
        for part in range(2):
            for b in range(beams_per_chunk):
                for block in range(blocks):
                    lanes = slice(block * LANES, (block + 1) * LANES)
                    tiles = [
                        chunk_buf[slot, part, row // SLAB, row % SLAB : row % SLAB + tall, lanes]
                        for row in range(b * antennas, (b + 1) * antennas, tall)
                    ]
                    if antennas < LANES:
                        tiles.append(jnp.zeros((LANES - antennas, LANES), jnp.float32))
                    row = block * LANES * w_stride + part * beams + n * beams_per_chunk + b
                    w_lines[pl.ds(row, LANES, stride=w_stride), :] = jnp.concatenate(tiles, axis=0).T * usable
        start_chunk(n + CHUNKS_IN_FLIGHT)

    def turn(h, first, last):
        @pl.loop(first, last)
        def _(m):
            n = w_chunks + h * x_chunks + m
            slot = slot_of(n)
            x_copy(h * x_chunks + m, slot).wait()
            for a in range(SLABS_PER_CHUNK):
                for block in range(blocks):
                    lanes = pl.ds(block * LANES, LANES)
                    tile = jnp.concatenate([chunk_buf[slot, part, a, :, lanes] for part in range(2)], axis=0)
                    row = block * LANES * x_stride + m * SLABS_PER_CHUNK + a
                    x_lines[h, pl.ds(row, LANES, stride=x_stride), :] = tile.T
            start_chunk(n + CHUNKS_IN_FLIGHT)

    turn(0, 0, x_chunks)

    pl.semaphore_wait(barrier, groups - 1 + stations - 1)
    for g in range(1, groups):
        count_copy(g).start()

    lane = lax.broadcasted_iota(jnp.int32, (beams, LANES), 1)
    sign = jnp.where(lane < SLAB, -1.0, 1.0).astype(jnp.float32)

    def partial(h, slot):
        f = table_ref[slot]
        x = x_rows[h, f, :antennas, :]
        w = w_rows[f, : 2 * beams, :antennas]
        x_pair = jnp.concatenate(split(x), axis=0)
        w_high, w_low = split(w)
        grid = jnp.dot(
            jnp.concatenate([w_high, w_high], axis=1), x_pair, preferred_element_type=jnp.float32
        ) + jnp.dot(jnp.concatenate([w_low, w_low], axis=1), x_pair, preferred_element_type=jnp.float32)
        return grid[:beams] + pltpu.roll(grid[beams:], SLAB, axis=1) * sign

    def peers(h, i):
        for g in range(1, groups):
            first = lax.rem(mine + g, groups) * kept + i * stations

            @pl.loop(0, parts_of_phase)
            def _(q):
                for u in range(GROUP):
                    total = partial(h, first + target(q * GROUP + u))
                    partials[g - 1, h, i, q, u] = total.astype(jnp.bfloat16)
                chan_copy(g, h, i, q).start()

    def own_sums(h, i):
        first = mine * kept + i * stations

        @pl.loop(0, parts_of_phase)
        def _(q):
            for u in range(GROUP):
                own[q, u] = partial(h, first + target(q * GROUP + u))

    def forward(h, i, gain):
        def piece(q, last):
            for g in range(1, groups):
                chan_copy(g, h, i, q).wait_recv()
            for u in range(GROUP):
                total = own[q, u]
                for g in range(1, groups):
                    total = total + arrived[g - 1, h, i, q, u].astype(jnp.float32)
                value = (total * gain).astype(jnp.bfloat16)
                if last and u == GROUP - 1:
                    gathered[h, i, me] = value
                else:
                    arrived[0, h, i, q, u] = value
                    beam_copy(h, i, q, u).start()

        @pl.loop(0, parts_of_phase - 1)
        def _(q):
            piece(q, False)

        piece(parts_of_phase - 1, True)

    tile_rows = stations * TILE_BEAMS
    mask = lax.broadcasted_iota(jnp.int32, (TILE_BEAMS, tile_rows), 0) == lax.rem(
        lax.broadcasted_iota(jnp.int32, (TILE_BEAMS, tile_rows), 1), TILE_BEAMS
    )
    chosen = mask.astype(jnp.float32).reshape(1, TILE_BEAMS, tile_rows)
    wide = tile_rows // LANES
    beam_tiles = beams // TILE_BEAMS
    result_rows = 2 * beam_tiles * wide

    def correlate(i):
        all_of(gathered.at[:, i, others], beam_send, beam_recv.at[i]).wait_recv()
        for tile in range(beam_tiles):
            straight, turned = [], []
            for h in range(halves):
                y = gathered[h, i, :, pl.ds(tile * TILE_BEAMS, TILE_BEAMS), :].reshape(tile_rows, LANES)
                straight.append(y)
                swapped = jnp.concatenate([y[:, SLAB:], -y[:, :SLAB]], axis=1)
                turned.append(swapped)
            y = jnp.concatenate(straight, axis=1)
            for part, x in enumerate((y, jnp.concatenate(turned, axis=1))):
                pairs = lax.dot_general(x, y, (((1,), (1,)), ((), ())), preferred_element_type=jnp.float32)
                total = jnp.sum(pairs.reshape(stations, TILE_BEAMS, tile_rows) * chosen, axis=1)
                for piece in range(wide):
                    row = (part * beam_tiles + tile) * wide + piece
                    results[i, :, row, :] = total[:, piece * LANES : (piece + 1) * LANES]

        far_results[i] = results[i, pl.ds(far_first, half)].astype(jnp.bfloat16)

        @pl.loop(0, half)
        def _(k):
            far_copy(i, k).start()

        @pl.loop(0, half - 1)
        def _(k):
            back_copy(i, k).start()

        returned[i * stations + me] = results[i, me]

    phases = halves * share
    ahead, behind = min(AHEAD, share), min(BEHIND, share)
    each = pl.cdiv(x_chunks, share - ahead + 1)

    for p in range(ahead):
        peers(0, p)
    count = count_ref[...]
    for g in range(1, groups):
        count_copy(g).wait_recv()
        count = count + counts[g - 1]
    gain = lax.rsqrt(count)[0:1, :]

    @pl.loop(0, phases)
    def _(p):
        turn(1, jnp.minimum(p * each, x_chunks * (halves - 1)), jnp.minimum((p + 1) * each, x_chunks * (halves - 1)))

        @pl.when(p + ahead < phases)
        def _():
            peers((p + ahead) // share, lax.rem(p + ahead, share))

        own_sums(p // share, lax.rem(p, share))
        forward(p // share, lax.rem(p, share), gain)

        @pl.when(p >= phases - share + behind)
        def _():
            correlate(p - (phases - share + behind))

    @pl.loop(share - behind, share)
    def _(i):
        correlate(i)

    all_of(returned.at[pl.ds(0, share * (half - 1))], back_send, back_recv).wait_recv()
    all_of(far_returned, far_send, far_recv).wait_recv()
    for i in range(share):
        returned[pl.ds(i * stations + far_first, half)] = far_returned[i].astype(jnp.float32)

    per_row = LANES // TILE_BEAMS
    for part in range(2):
        for tile in range(beam_tiles):
            for piece in range(wide):
                row = (part * beam_tiles + tile) * wide + piece
                turned = returned[:, row, :].T
                for r in range(per_row):
                    out_ref[part, pl.ds(tile * TILE_BEAMS, TILE_BEAMS), piece * per_row + r, :] = turned[
                        r * TILE_BEAMS : (r + 1) * TILE_BEAMS
                    ]

    for g in range(1, groups):
        count_copy(g).wait_send()
    all_of(partials, chan_send, chan_recv.at[0, 0, 0, 0]).wait_send()
    all_of(gathered.at[:, :, others], beam_send, beam_recv.at[0]).wait_send()
    all_of(results.at[:, pl.ds(0, half - 1)], back_send, back_recv).wait_send()
    all_of(far_results, far_send, far_recv).wait_send()


def on_device(samples, weights, antenna_flags, subband_table):
    groups, stations = lax.axis_size("chan"), lax.axis_size("station")
    _, _, antennas, times, subbands = samples.shape
    beams = weights.shape[2]
    kept = subbands // groups
    share = kept // stations
    halves = times // SLAB
    quarters = stations // GROUP
    rows = 2 * (beams // TILE_BEAMS) * (stations * TILE_BEAMS // LANES)
    slabs = weights.reshape(2, 1, beams * antennas // SLAB, SLAB, subbands)
    dma = pltpu.SemaphoreType.DMA
    out = pl.pallas_call(
        kernel,
        out_shape=jax.ShapeDtypeStruct((2, beams, stations, kept), jnp.float32),
        in_specs=[
            pl.BlockSpec(memory_space=pltpu.SMEM),
            pl.BlockSpec(memory_space=pltpu.VMEM),
            pl.BlockSpec(memory_space=pl.ANY),
            pl.BlockSpec(memory_space=pl.ANY),
        ],
        out_specs=pl.BlockSpec(memory_space=pltpu.VMEM),
        scratch_shapes=[
            pltpu.VMEM((halves, subbands, antennas + 8, LANES), jnp.float32),
            pltpu.VMEM((subbands, 2 * beams + 8, LANES), jnp.float32),
            pltpu.VMEM((CHUNKS_IN_FLIGHT, 2, SLABS_PER_CHUNK, SLAB, subbands), jnp.float32),
            pltpu.VMEM((quarters, GROUP, beams, LANES), jnp.float32),
            pltpu.VMEM((groups - 1, halves, share, quarters, GROUP, beams, LANES), jnp.bfloat16),
            pltpu.VMEM((groups - 1, halves, share, quarters, GROUP, beams, LANES), jnp.bfloat16),
            pltpu.VMEM((halves, share, stations, beams, LANES), jnp.bfloat16),
            pltpu.VMEM((share, stations, rows, LANES), jnp.float32),
            pltpu.VMEM((share, stations // 2, rows, LANES), jnp.bfloat16),
            pltpu.VMEM((kept, rows, LANES), jnp.float32),
            pltpu.VMEM((share, stations // 2, rows, LANES), jnp.bfloat16),
            pltpu.VMEM((8, LANES), jnp.float32),
            pltpu.VMEM((groups - 1, 8, LANES), jnp.float32),
            dma((CHUNKS_IN_FLIGHT,)),
            dma((groups - 1,)),
            dma((groups - 1,)),
            dma,
            dma((groups - 1, halves, share, quarters)),
            dma,
            dma((share,)),
            dma,
            dma,
            dma,
            dma,
        ],
        compiler_params=pltpu.CompilerParams(
            collective_id=0, has_side_effects=True, vmem_limit_bytes=67043328
        ),
    )(subband_table, antenna_flags, samples, slabs)
    return out.transpose(3, 0, 1, 2)[:, :, None]


def solution(mesh):
    in_specs = (
        P(None, "station", "chan", None, None),
        P(None, "station", None, "chan", None),
        P("station", "chan"),
        P(),
    )
    out_specs = P("chan", None, "station", None, None)
    return jax.shard_map(
        on_device, mesh=mesh, in_specs=in_specs, out_specs=out_specs, check_vma=False
    )
```

```python
import functools

import jax
import jax.numpy as jnp
from jax import lax
from jax.experimental import pallas as pl
from jax.experimental.pallas import tpu as pltpu
from jax.sharding import PartitionSpec as P

LANES = 128
SLAB = 64
SLABS_PER_CHUNK = 8
CHUNKS_IN_FLIGHT = 8
GROUP = 8
TILE_BEAMS = 16
AHEAD = 3
BEHIND = 3


def split(value):
    high = value.astype(jnp.bfloat16)
    low = (value - high.astype(jnp.float32)).astype(jnp.bfloat16)
    return high, low


def kernel(
    table_ref, flags_ref, x_hbm, w_hbm, out_ref,
    x_rows, w_rows, chunk_buf, own, partials, arrived, gathered, results, far_results, returned, far_returned, count_ref, counts,
    chunk_sem, count_send, count_recv, chan_send, chan_recv, beam_send, beam_recv, back_send, back_recv,
    far_send, far_recv,
):
    groups, stations = lax.axis_size("chan"), lax.axis_size("station")
    mine, me = lax.axis_index("chan"), lax.axis_index("station")
    halves, share = gathered.shape[0], gathered.shape[1]
    antennas = x_hbm.shape[2]
    subbands = x_hbm.shape[4]
    beams = gathered.shape[3]
    kept = subbands // groups
    blocks = subbands // LANES
    tall = min(antennas, SLAB)
    x_stride = x_rows.shape[2]
    w_stride = w_rows.shape[1]
    w_chunks = w_hbm.shape[2] // SLABS_PER_CHUNK
    x_chunks = antennas // SLABS_PER_CHUNK
    chunks = w_chunks + halves * x_chunks
    beams_per_chunk = SLABS_PER_CHUNK * SLAB // antennas
    parts_of_phase = stations // GROUP
    x_lines = x_rows.reshape(halves, subbands * x_stride, LANES)
    w_lines = w_rows.reshape(subbands * w_stride, LANES)

    def target(k):
        return lax.rem(me + stations // 2 + ((k + 1) // 2) * (1 - 2 * lax.rem(k, 2)), stations)

    def remote(src, dst, send, recv, device):
        return pltpu.make_async_remote_copy(
            src_ref=src, dst_ref=dst, send_sem=send, recv_sem=recv,
            device_id=device, device_id_type=pl.DeviceIdType.MESH,
        )

    def chan_copy(g, h, i, q):
        peer = lax.rem(mine + g, groups)
        return remote(
            partials.at[g - 1, h, i, q], arrived.at[g - 1, h, i, q],
            chan_send, chan_recv.at[g - 1, h, i, q], (me, peer),
        )

    def count_copy(g):
        return remote(
            count_ref, counts.at[g - 1], count_send.at[g - 1], count_recv.at[g - 1], (me, lax.rem(mine + g, groups))
        )

    def beam_copy(h, i, q, u):
        return remote(
            arrived.at[0, h, i, q, u], gathered.at[h, i, me],
            beam_send, beam_recv.at[i], (target(q * GROUP + u), mine),
        )

    half = stations // 2
    near_first = me // half * half
    far_first = half - near_first

    def back_copy(i, k):
        there = near_first + lax.rem(me + 1 + k, half)
        return remote(
            results.at[i, there], returned.at[i * stations + me], back_send, back_recv, (there, mine)
        )

    def far_copy(i, k):
        return remote(
            far_results.at[i, k], far_returned.at[i, lax.rem(me, half)], far_send, far_recv,
            (far_first + k, mine),
        )

    def all_of(ref, send, recv):
        return remote(ref, ref, send, recv, (me, lax.rem(mine + 1, groups)))

    others = pl.ds(0, stations - 1)

    def w_copy(n, slot):
        return pltpu.make_async_copy(
            w_hbm.at[:, 0, pl.ds(n * SLABS_PER_CHUNK, SLABS_PER_CHUNK)], chunk_buf.at[slot], chunk_sem.at[slot]
        )

    def x_copy(n, slot):
        half = n // x_chunks
        first = lax.rem(n, x_chunks) * SLABS_PER_CHUNK
        return pltpu.make_async_copy(
            x_hbm.at[:, 0, pl.ds(first, SLABS_PER_CHUNK), pl.ds(half * SLAB, SLAB)],
            chunk_buf.at[slot], chunk_sem.at[slot],
        )

    def slot_of(n):
        return lax.rem(n, CHUNKS_IN_FLIGHT)

    def start_chunk(n):
        @pl.when(n < w_chunks)
        def _():
            w_copy(n, slot_of(n)).start()

        @pl.when((n >= w_chunks) & (n < chunks))
        def _():
            x_copy(n - w_chunks, slot_of(n)).start()

    for n in range(min(CHUNKS_IN_FLIGHT, chunks)):
        if n < w_chunks:
            w_copy(n, n % CHUNKS_IN_FLIGHT).start()
        else:
            x_copy(n - w_chunks, n % CHUNKS_IN_FLIGHT).start()

    barrier = pltpu.get_barrier_semaphore()
    for g in range(1, groups):
        pl.semaphore_signal(
            barrier, inc=1, device_id=(me, lax.rem(mine + g, groups)), device_id_type=pl.DeviceIdType.MESH
        )

    @pl.loop(0, stations - 1)
    def _(k):
        pl.semaphore_signal(barrier, inc=1, device_id=(target(k), mine), device_id_type=pl.DeviceIdType.MESH)

    usable = flags_ref[...].astype(jnp.float32)
    count_ref[...] = jnp.broadcast_to(jnp.sum(usable, axis=1, keepdims=True), count_ref.shape)
    if antennas < LANES:
        usable = jnp.concatenate([usable, jnp.zeros((1, LANES - antennas), jnp.float32)], axis=1)

    @pl.loop(0, w_chunks)
    def _(n):
        slot = slot_of(n)
        w_copy(n, slot).wait()
        for part in range(2):
            for b in range(beams_per_chunk):
                for block in range(blocks):
                    lanes = slice(block * LANES, (block + 1) * LANES)
                    tiles = [
                        chunk_buf[slot, part, row // SLAB, row % SLAB : row % SLAB + tall, lanes]
                        for row in range(b * antennas, (b + 1) * antennas, tall)
                    ]
                    if antennas < LANES:
                        tiles.append(jnp.zeros((LANES - antennas, LANES), jnp.float32))
                    row = block * LANES * w_stride + part * beams + n * beams_per_chunk + b
                    w_lines[pl.ds(row, LANES, stride=w_stride), :] = jnp.concatenate(tiles, axis=0).T * usable
        start_chunk(n + CHUNKS_IN_FLIGHT)

    def turn(h, first, last):
        @pl.loop(first, last)
        def _(m):
            n = w_chunks + h * x_chunks + m
            slot = slot_of(n)
            x_copy(h * x_chunks + m, slot).wait()
            for a in range(SLABS_PER_CHUNK):
                for block in range(blocks):
                    lanes = pl.ds(block * LANES, LANES)
                    tile = jnp.concatenate([chunk_buf[slot, part, a, :, lanes] for part in range(2)], axis=0)
                    row = block * LANES * x_stride + m * SLABS_PER_CHUNK + a
                    x_lines[h, pl.ds(row, LANES, stride=x_stride), :] = tile.T
            start_chunk(n + CHUNKS_IN_FLIGHT)

    turn(0, 0, x_chunks)

    pl.semaphore_wait(barrier, groups - 1 + stations - 1)
    for g in range(1, groups):
        count_copy(g).start()

    lane = lax.broadcasted_iota(jnp.int32, (beams, LANES), 1)
    sign = jnp.where(lane < SLAB, -1.0, 1.0).astype(jnp.float32)

    def partial(h, slot):
        f = table_ref[slot]
        x = x_rows[h, f, :antennas, :]
        w = w_rows[f, : 2 * beams, :antennas]
        x_pair = jnp.concatenate(split(x), axis=0)
        w_high, w_low = split(w)
        grid = jnp.dot(
            jnp.concatenate([w_high, w_high], axis=1), x_pair, preferred_element_type=jnp.float32
        ) + jnp.dot(jnp.concatenate([w_low, w_low], axis=1), x_pair, preferred_element_type=jnp.float32)
        return grid[:beams] + pltpu.roll(grid[beams:], SLAB, axis=1) * sign

    def peers(h, i):
        for g in range(1, groups):
            first = lax.rem(mine + g, groups) * kept + i * stations

            @pl.loop(0, parts_of_phase)
            def _(q):
                for u in range(GROUP):
                    total = partial(h, first + target(q * GROUP + u))
                    partials[g - 1, h, i, q, u] = total.astype(jnp.bfloat16)
                chan_copy(g, h, i, q).start()

    def own_sums(h, i):
        first = mine * kept + i * stations

        @pl.loop(0, parts_of_phase)
        def _(q):
            for u in range(GROUP):
                own[q, u] = partial(h, first + target(q * GROUP + u))

    def forward(h, i, gain):
        def piece(q, last):
            for g in range(1, groups):
                chan_copy(g, h, i, q).wait_recv()
            for u in range(GROUP):
                total = own[q, u]
                for g in range(1, groups):
                    total = total + arrived[g - 1, h, i, q, u].astype(jnp.float32)
                value = (total * gain).astype(jnp.bfloat16)
                if last and u == GROUP - 1:
                    gathered[h, i, me] = value
                else:
                    arrived[0, h, i, q, u] = value
                    beam_copy(h, i, q, u).start()

        @pl.loop(0, parts_of_phase - 1)
        def _(q):
            piece(q, False)

        piece(parts_of_phase - 1, True)

    tile_rows = stations * TILE_BEAMS
    mask = lax.broadcasted_iota(jnp.int32, (TILE_BEAMS, tile_rows), 0) == lax.rem(
        lax.broadcasted_iota(jnp.int32, (TILE_BEAMS, tile_rows), 1), TILE_BEAMS
    )
    chosen = mask.astype(jnp.float32).reshape(1, TILE_BEAMS, tile_rows)
    wide = tile_rows // LANES
    beam_tiles = beams // TILE_BEAMS
    result_rows = 2 * beam_tiles * wide

    def spare(shape, station):
        row, place = lax.broadcasted_iota(jnp.int32, shape, 1), lax.broadcasted_iota(jnp.int32, shape, 2)
        other = lax.rem(row, wide) * (LANES // TILE_BEAMS) + place // TILE_BEAMS
        return (row >= result_rows // 2) & (other == station)

    def correlate(i):
        all_of(gathered.at[:, i, others], beam_send, beam_recv.at[i]).wait_recv()
        for tile in range(beam_tiles):
            straight, turned = [], []
            for h in range(halves):
                y = gathered[h, i, :, pl.ds(tile * TILE_BEAMS, TILE_BEAMS), :].reshape(tile_rows, LANES)
                straight.append(y)
                swapped = jnp.concatenate([y[:, SLAB:], -y[:, :SLAB]], axis=1)
                turned.append(swapped)
            y = jnp.concatenate(straight, axis=1)
            for part, x in enumerate((y, jnp.concatenate(turned, axis=1))):
                pairs = lax.dot_general(x, y, (((1,), (1,)), ((), ())), preferred_element_type=jnp.float32)
                total = jnp.sum(pairs.reshape(stations, TILE_BEAMS, tile_rows) * chosen, axis=1)
                for piece in range(wide):
                    row = (part * beam_tiles + tile) * wide + piece
                    results[i, :, row, :] = total[:, piece * LANES : (piece + 1) * LANES]

        value = results[i, pl.ds(far_first, half)]
        low = value - value.astype(jnp.bfloat16).astype(jnp.float32)
        station = far_first + lax.broadcasted_iota(jnp.int32, value.shape, 0)
        far_results[i] = jnp.where(
            spare(value.shape, station), pltpu.roll(low, result_rows // 2, axis=1), value
        ).astype(jnp.bfloat16)

        @pl.loop(0, half)
        def _(k):
            far_copy(i, k).start()

        @pl.loop(0, half - 1)
        def _(k):
            back_copy(i, k).start()

        returned[i * stations + me] = results[i, me]

    phases = halves * share
    ahead, behind = min(AHEAD, share), min(BEHIND, share)
    each = pl.cdiv(x_chunks, share - ahead + 1)

    for p in range(ahead):
        peers(0, p)
    count = count_ref[...]
    for g in range(1, groups):
        count_copy(g).wait_recv()
        count = count + counts[g - 1]
    gain = lax.rsqrt(count)[0:1, :]

    @pl.loop(0, phases)
    def _(p):
        turn(1, jnp.minimum(p * each, x_chunks * (halves - 1)), jnp.minimum((p + 1) * each, x_chunks * (halves - 1)))

        @pl.when(p + ahead < phases)
        def _():
            peers((p + ahead) // share, lax.rem(p + ahead, share))

        own_sums(p // share, lax.rem(p, share))
        forward(p // share, lax.rem(p, share), gain)

        @pl.when(p >= phases - share + behind)
        def _():
            correlate(p - (phases - share + behind))

    @pl.loop(share - behind, share)
    def _(i):
        correlate(i)

    all_of(returned.at[pl.ds(0, share * (half - 1))], back_send, back_recv).wait_recv()
    all_of(far_returned, far_send, far_recv).wait_recv()
    for i in range(share):
        value = far_returned[i].astype(jnp.float32)
        extra = spare(value.shape, me)
        low = pltpu.roll(jnp.where(extra, value, 0.0), result_rows // 2, axis=1)
        returned[pl.ds(i * stations + far_first, half)] = jnp.where(extra, 0.0, value + low)

    per_row = LANES // TILE_BEAMS
    for part in range(2):
        for tile in range(beam_tiles):
            for piece in range(wide):
                row = (part * beam_tiles + tile) * wide + piece
                turned = returned[:, row, :].T
                for r in range(per_row):
                    out_ref[part, pl.ds(tile * TILE_BEAMS, TILE_BEAMS), piece * per_row + r, :] = turned[
                        r * TILE_BEAMS : (r + 1) * TILE_BEAMS
                    ]

    for g in range(1, groups):
        count_copy(g).wait_send()
    all_of(partials, chan_send, chan_recv.at[0, 0, 0, 0]).wait_send()
    all_of(gathered.at[:, :, others], beam_send, beam_recv.at[0]).wait_send()
    all_of(results.at[:, pl.ds(0, half - 1)], back_send, back_recv).wait_send()
    all_of(far_results, far_send, far_recv).wait_send()


def on_device(samples, weights, antenna_flags, subband_table):
    groups, stations = lax.axis_size("chan"), lax.axis_size("station")
    _, _, antennas, times, subbands = samples.shape
    beams = weights.shape[2]
    kept = subbands // groups
    share = kept // stations
    halves = times // SLAB
    quarters = stations // GROUP
    rows = 2 * (beams // TILE_BEAMS) * (stations * TILE_BEAMS // LANES)
    slabs = weights.reshape(2, 1, beams * antennas // SLAB, SLAB, subbands)
    dma = pltpu.SemaphoreType.DMA
    out = pl.pallas_call(
        kernel,
        out_shape=jax.ShapeDtypeStruct((2, beams, stations, kept), jnp.float32),
        in_specs=[
            pl.BlockSpec(memory_space=pltpu.SMEM),
            pl.BlockSpec(memory_space=pltpu.VMEM),
            pl.BlockSpec(memory_space=pl.ANY),
            pl.BlockSpec(memory_space=pl.ANY),
        ],
        out_specs=pl.BlockSpec(memory_space=pltpu.VMEM),
        scratch_shapes=[
            pltpu.VMEM((halves, subbands, antennas + 8, LANES), jnp.float32),
            pltpu.VMEM((subbands, 2 * beams + 8, LANES), jnp.float32),
            pltpu.VMEM((CHUNKS_IN_FLIGHT, 2, SLABS_PER_CHUNK, SLAB, subbands), jnp.float32),
            pltpu.VMEM((quarters, GROUP, beams, LANES), jnp.float32),
            pltpu.VMEM((groups - 1, halves, share, quarters, GROUP, beams, LANES), jnp.bfloat16),
            pltpu.VMEM((groups - 1, halves, share, quarters, GROUP, beams, LANES), jnp.bfloat16),
            pltpu.VMEM((halves, share, stations, beams, LANES), jnp.bfloat16),
            pltpu.VMEM((share, stations, rows, LANES), jnp.float32),
            pltpu.VMEM((share, stations // 2, rows, LANES), jnp.bfloat16),
            pltpu.VMEM((kept, rows, LANES), jnp.float32),
            pltpu.VMEM((share, stations // 2, rows, LANES), jnp.bfloat16),
            pltpu.VMEM((8, LANES), jnp.float32),
            pltpu.VMEM((groups - 1, 8, LANES), jnp.float32),
            dma((CHUNKS_IN_FLIGHT,)),
            dma((groups - 1,)),
            dma((groups - 1,)),
            dma,
            dma((groups - 1, halves, share, quarters)),
            dma,
            dma((share,)),
            dma,
            dma,
            dma,
            dma,
        ],
        compiler_params=pltpu.CompilerParams(
            collective_id=0, has_side_effects=True, vmem_limit_bytes=67043328
        ),
    )(subband_table, antenna_flags, samples, slabs)
    return out.transpose(3, 0, 1, 2)[:, :, None]


def solution(mesh):
    in_specs = (
        P(None, "station", "chan", None, None),
        P(None, "station", None, "chan", None),
        P("station", "chan"),
        P(),
    )
    out_specs = P("chan", None, "station", None, None)
    return jax.shard_map(
        on_device, mesh=mesh, in_specs=in_specs, out_specs=out_specs, check_vma=False
    )
```

```python
import functools

import jax
import jax.numpy as jnp
from jax import lax
from jax.experimental import pallas as pl
from jax.experimental.pallas import tpu as pltpu
from jax.sharding import PartitionSpec as P

LANES = 128
SLAB = 64
SLABS_PER_CHUNK = 8
CHUNKS_IN_FLIGHT = 5
GROUP = 8
UNROLL = 16
TILE_BEAMS = 16
AHEAD = 3
BEHIND = 3


def split(value):
    high = value.astype(jnp.bfloat16)
    low = (value - high.astype(jnp.float32)).astype(jnp.bfloat16)
    return high, low


def kernel(
    table_hbm, flags_hbm, x_hbm, w_hbm, out_ref,
    table_ref, flags_ref, rows, chunk_buf, own, partials, arrived, gathered, results, far_results, returned, far_returned, count_ref, counts,
    small_sem, chunk_sem, count_send, count_recv, chan_send, chan_recv, beam_send, beam_recv, back_send, back_recv,
    far_send, far_recv,
):
    groups, stations = lax.axis_size("chan"), lax.axis_size("station")
    mine, me = lax.axis_index("chan"), lax.axis_index("station")
    halves, share = gathered.shape[0], gathered.shape[1]
    antennas = x_hbm.shape[2]
    subbands = x_hbm.shape[4]
    beams = gathered.shape[3]
    kept = subbands // groups
    blocks = subbands // LANES
    tall = min(antennas, SLAB)
    stride = rows.shape[1]
    w_first = halves * antennas
    w_chunks = w_hbm.shape[2] // SLABS_PER_CHUNK
    x_chunks = antennas // SLABS_PER_CHUNK
    chunks = w_chunks + halves * x_chunks
    beams_per_chunk = SLABS_PER_CHUNK * SLAB // antennas
    parts_of_phase = stations // GROUP
    lines = rows.reshape(subbands * stride, LANES)

    def target(k):
        return lax.rem(me + stations // 2 + ((k + 1) // 2) * (1 - 2 * lax.rem(k, 2)), stations)

    def remote(src, dst, send, recv, device):
        return pltpu.make_async_remote_copy(
            src_ref=src, dst_ref=dst, send_sem=send, recv_sem=recv,
            device_id=device, device_id_type=pl.DeviceIdType.MESH,
        )

    def chan_copy(g, h, i, q):
        peer = lax.rem(mine + g, groups)
        return remote(
            partials.at[g - 1, h, i, q], arrived.at[g - 1, h, i, q],
            chan_send, chan_recv.at[g - 1, h, i, q], (me, peer),
        )

    def count_copy(g):
        return remote(
            count_ref, counts.at[g - 1], count_send.at[g - 1], count_recv.at[g - 1], (me, lax.rem(mine + g, groups))
        )

    def beam_copy(h, i, q, u):
        return remote(
            arrived.at[0, h, i, q, u], gathered.at[h, i, me],
            beam_send, beam_recv.at[i], (target(q * GROUP + u), mine),
        )

    half = stations // 2
    near_first = me // half * half
    far_first = half - near_first

    def back_copy(i, k):
        there = near_first + lax.rem(me + 1 + k, half)
        return remote(
            results.at[i, there], returned.at[i, lax.rem(me, half)], back_send, back_recv, (there, mine)
        )

    def far_copy(i, k):
        return remote(
            far_results.at[i, k], far_returned.at[i, lax.rem(me, half)], far_send, far_recv,
            (far_first + k, mine),
        )

    def all_of(ref, send, recv):
        return remote(ref, ref, send, recv, (me, lax.rem(mine + 1, groups)))

    others = pl.ds(0, stations - 1)

    def w_copy(n, slot):
        return pltpu.make_async_copy(
            w_hbm.at[:, 0, pl.ds(n * SLABS_PER_CHUNK, SLABS_PER_CHUNK)], chunk_buf.at[slot], chunk_sem.at[slot]
        )

    def x_copy(n, slot):
        half = n // x_chunks
        first = lax.rem(n, x_chunks) * SLABS_PER_CHUNK
        return pltpu.make_async_copy(
            x_hbm.at[:, 0, pl.ds(first, SLABS_PER_CHUNK), pl.ds(half * SLAB, SLAB)],
            chunk_buf.at[slot], chunk_sem.at[slot],
        )

    def slot_of(n):
        return lax.rem(n, CHUNKS_IN_FLIGHT)

    def start_chunk(n):
        @pl.when(n < w_chunks)
        def _():
            w_copy(n, slot_of(n)).start()

        @pl.when((n >= w_chunks) & (n < chunks))
        def _():
            x_copy(n - w_chunks, slot_of(n)).start()

    flags_copy = pltpu.make_async_copy(flags_hbm, flags_ref, small_sem.at[0])
    table_copy = pltpu.make_async_copy(table_hbm, table_ref, small_sem.at[1])
    flags_copy.start()
    table_copy.start()
    for n in range(min(CHUNKS_IN_FLIGHT, chunks)):
        if n < w_chunks:
            w_copy(n, n % CHUNKS_IN_FLIGHT).start()
        else:
            x_copy(n - w_chunks, n % CHUNKS_IN_FLIGHT).start()

    barrier = pltpu.get_barrier_semaphore()
    for g in range(1, groups):
        pl.semaphore_signal(
            barrier, inc=1, device_id=(me, lax.rem(mine + g, groups)), device_id_type=pl.DeviceIdType.MESH
        )

    @pl.loop(0, stations - 1)
    def _(k):
        pl.semaphore_signal(barrier, inc=1, device_id=(target(k), mine), device_id_type=pl.DeviceIdType.MESH)

    flags_copy.wait()
    usable = flags_ref[...].astype(jnp.float32)
    count_ref[...] = jnp.broadcast_to(jnp.sum(usable, axis=1, keepdims=True), count_ref.shape)
    if antennas < LANES:
        usable = jnp.concatenate([usable, jnp.zeros((1, LANES - antennas), jnp.float32)], axis=1)

    @pl.loop(0, w_chunks)
    def _(n):
        slot = slot_of(n)
        w_copy(n, slot).wait()
        for part in range(2):
            for b in range(beams_per_chunk):
                for block in range(blocks):
                    lanes = slice(block * LANES, (block + 1) * LANES)
                    tiles = [
                        chunk_buf[slot, part, row // SLAB, row % SLAB : row % SLAB + tall, lanes]
                        for row in range(b * antennas, (b + 1) * antennas, tall)
                    ]
                    if antennas < LANES:
                        tiles.append(jnp.zeros((LANES - antennas, LANES), jnp.float32))
                    row = block * LANES * stride + w_first + part * beams + n * beams_per_chunk + b
                    lines[pl.ds(row, LANES, stride=stride), :] = jnp.concatenate(tiles, axis=0).T * usable
        start_chunk(n + CHUNKS_IN_FLIGHT)

    def turn(h, first, last):
        @pl.loop(first, last)
        def _(m):
            n = w_chunks + h * x_chunks + m
            slot = slot_of(n)
            x_copy(h * x_chunks + m, slot).wait()
            for a in range(SLABS_PER_CHUNK):
                for block in range(blocks):
                    lanes = pl.ds(block * LANES, LANES)
                    tile = jnp.concatenate([chunk_buf[slot, part, a, :, lanes] for part in range(2)], axis=0)
                    row = block * LANES * stride + h * antennas + m * SLABS_PER_CHUNK + a
                    lines[pl.ds(row, LANES, stride=stride), :] = tile.T
            start_chunk(n + CHUNKS_IN_FLIGHT)

    turn(0, 0, x_chunks)

    table_copy.wait()
    pl.semaphore_wait(barrier, groups - 1 + stations - 1)
    for g in range(1, groups):
        count_copy(g).start()

    lane = lax.broadcasted_iota(jnp.int32, (beams, LANES), 1)
    sign = jnp.where(lane < SLAB, -1.0, 1.0).astype(jnp.float32)

    def partial(h, slot):
        f = table_ref[slot]
        x = rows[f, pl.ds(pl.multiple_of(h * antennas, 8), antennas), :]
        w = rows[f, w_first : w_first + 2 * beams, :antennas]
        x_pair = jnp.concatenate(split(x), axis=0)
        w_high, w_low = split(w)
        grid = jnp.dot(
            jnp.concatenate([w_high, w_high], axis=1), x_pair, preferred_element_type=jnp.float32
        ) + jnp.dot(jnp.concatenate([w_low, w_low], axis=1), x_pair, preferred_element_type=jnp.float32)
        return grid[:beams] + pltpu.roll(grid[beams:], SLAB, axis=1) * sign

    def peers(h, i):
        for g in range(1, groups):
            first = lax.rem(mine + g, groups) * kept + i * stations

            @pl.loop(0, stations // UNROLL)
            def _(v):
                for w in range(UNROLL // GROUP):
                    q = v * (UNROLL // GROUP) + w
                    for u in range(GROUP):
                        total = partial(h, first + target(q * GROUP + u))
                        partials[g - 1, h, i, q, u] = total.astype(jnp.bfloat16)
                    chan_copy(g, h, i, q).start()

    def own_sums(h, i):
        first = mine * kept + i * stations

        @pl.loop(0, stations // UNROLL)
        def _(v):
            for w in range(UNROLL // GROUP):
                q = v * (UNROLL // GROUP) + w
                for u in range(GROUP):
                    own[q, u] = partial(h, first + target(q * GROUP + u))

    def forward(h, i, gain):
        def piece(q, last):
            for g in range(1, groups):
                chan_copy(g, h, i, q).wait_recv()
            for u in range(GROUP):
                total = own[q, u]
                for g in range(1, groups):
                    total = total + arrived[g - 1, h, i, q, u].astype(jnp.float32)
                value = (total * gain).astype(jnp.bfloat16)
                if last and u == GROUP - 1:
                    gathered[h, i, me] = value
                else:
                    arrived[0, h, i, q, u] = value
                    beam_copy(h, i, q, u).start()

        @pl.loop(0, parts_of_phase - 1)
        def _(q):
            piece(q, False)

        piece(parts_of_phase - 1, True)

    tile_rows = stations * TILE_BEAMS
    mask = lax.broadcasted_iota(jnp.int32, (TILE_BEAMS, tile_rows), 0) == lax.rem(
        lax.broadcasted_iota(jnp.int32, (TILE_BEAMS, tile_rows), 1), TILE_BEAMS
    )
    chosen = mask.astype(jnp.float32).reshape(1, TILE_BEAMS, tile_rows)
    wide = tile_rows // LANES
    beam_tiles = beams // TILE_BEAMS
    result_rows = 2 * beam_tiles * wide

    def spare(shape, station):
        row, place = lax.broadcasted_iota(jnp.int32, shape, 1), lax.broadcasted_iota(jnp.int32, shape, 2)
        other = lax.rem(row, wide) * (LANES // TILE_BEAMS) + place // TILE_BEAMS
        return (row >= result_rows // 2) & (other == station)

    def correlate(i):
        all_of(gathered.at[:, i, others], beam_send, beam_recv.at[i]).wait_recv()
        for tile in range(beam_tiles):
            straight, turned = [], []
            for h in range(halves):
                y = gathered[h, i, :, pl.ds(tile * TILE_BEAMS, TILE_BEAMS), :].reshape(tile_rows, LANES)
                straight.append(y)
                swapped = jnp.concatenate([y[:, SLAB:], -y[:, :SLAB]], axis=1)
                turned.append(swapped)
            y = jnp.concatenate(straight, axis=1)
            for part, x in enumerate((y, jnp.concatenate(turned, axis=1))):
                pairs = lax.dot_general(x, y, (((1,), (1,)), ((), ())), preferred_element_type=jnp.float32)
                total = jnp.sum(pairs.reshape(stations, TILE_BEAMS, tile_rows) * chosen, axis=1)
                for piece in range(wide):
                    row = (part * beam_tiles + tile) * wide + piece
                    results[i, :, row, :] = total[:, piece * LANES : (piece + 1) * LANES]

        value = results[i, pl.ds(far_first, half)]
        low = value - value.astype(jnp.bfloat16).astype(jnp.float32)
        station = far_first + lax.broadcasted_iota(jnp.int32, value.shape, 0)
        far_results[i] = jnp.where(
            spare(value.shape, station), pltpu.roll(low, result_rows // 2, axis=1), value
        ).astype(jnp.bfloat16)

        @pl.loop(0, half)
        def _(k):
            far_copy(i, k).start()

        @pl.loop(0, half - 1)
        def _(k):
            back_copy(i, k).start()

        returned[i, lax.rem(me, half)] = results[i, me]

    phases = halves * share
    ahead, behind = min(AHEAD, share), min(BEHIND, share)
    each = pl.cdiv(x_chunks, share - ahead + 1)

    for p in range(ahead):
        peers(0, p)
    count = count_ref[...]
    for g in range(1, groups):
        count_copy(g).wait_recv()
        count = count + counts[g - 1]
    gain = lax.rsqrt(count)[0:1, :]

    @pl.loop(0, phases)
    def _(p):
        own_sums(p // share, lax.rem(p, share))
        forward(p // share, lax.rem(p, share), gain)

        turn(1, jnp.minimum(p * each, x_chunks * (halves - 1)), jnp.minimum((p + 1) * each, x_chunks * (halves - 1)))

        @pl.when(p + ahead < phases)
        def _():
            peers((p + ahead) // share, lax.rem(p + ahead, share))

        @pl.when(p >= phases - share + behind)
        def _():
            correlate(p - (phases - share + behind))

    @pl.loop(share - behind, share)
    def _(i):
        correlate(i)

    all_of(returned.at[:, pl.ds(0, half - 1)], back_send, back_recv).wait_recv()
    all_of(results.at[:, pl.ds(0, half - 1)], back_send, back_recv).wait_send()
    all_of(far_returned, far_send, far_recv).wait_recv()
    for i in range(share):
        value = far_returned[i].astype(jnp.float32)
        extra = spare(value.shape, me)
        low = pltpu.roll(jnp.where(extra, value, 0.0), result_rows // 2, axis=1)
        results[i, pl.ds(far_first, half)] = jnp.where(extra, 0.0, value + low)
        results[i, pl.ds(near_first, half)] = returned[i]

    per_row = LANES // TILE_BEAMS
    for part in range(2):
        for tile in range(beam_tiles):
            for piece in range(wide):
                row = (part * beam_tiles + tile) * wide + piece
                turned = results[:, :, row, :].reshape(kept, LANES).T
                for r in range(per_row):
                    out_ref[part, pl.ds(tile * TILE_BEAMS, TILE_BEAMS), piece * per_row + r, :] = turned[
                        r * TILE_BEAMS : (r + 1) * TILE_BEAMS
                    ]

    for g in range(1, groups):
        count_copy(g).wait_send()
    all_of(partials, chan_send, chan_recv.at[0, 0, 0, 0]).wait_send()
    all_of(gathered.at[:, :, others], beam_send, beam_recv.at[0]).wait_send()
    all_of(far_results, far_send, far_recv).wait_send()


def on_device(samples, weights, antenna_flags, subband_table):
    groups, stations = lax.axis_size("chan"), lax.axis_size("station")
    _, _, antennas, times, subbands = samples.shape
    beams = weights.shape[2]
    kept = subbands // groups
    share = kept // stations
    halves = times // SLAB
    quarters = stations // GROUP
    result_rows = 2 * (beams // TILE_BEAMS) * (stations * TILE_BEAMS // LANES)
    slabs = weights.reshape(2, 1, beams * antennas // SLAB, SLAB, subbands)
    dma = pltpu.SemaphoreType.DMA
    out = pl.pallas_call(
        kernel,
        out_shape=jax.ShapeDtypeStruct((2, beams, stations, kept), jnp.float32),
        in_specs=[
            pl.BlockSpec(memory_space=pltpu.HBM),
            pl.BlockSpec(memory_space=pltpu.HBM),
            pl.BlockSpec(memory_space=pl.ANY),
            pl.BlockSpec(memory_space=pl.ANY),
        ],
        out_specs=pl.BlockSpec(memory_space=pltpu.VMEM),
        scratch_shapes=[
            pltpu.SMEM((subbands,), jnp.int32),
            pltpu.VMEM((1, antennas), jnp.int32),
            pltpu.VMEM((subbands, halves * antennas + 2 * beams + 8, LANES), jnp.float32),
            pltpu.VMEM((CHUNKS_IN_FLIGHT, 2, SLABS_PER_CHUNK, SLAB, subbands), jnp.float32),
            pltpu.VMEM((quarters, GROUP, beams, LANES), jnp.float32),
            pltpu.VMEM((groups - 1, halves, share, quarters, GROUP, beams, LANES), jnp.bfloat16),
            pltpu.VMEM((groups - 1, halves, share, quarters, GROUP, beams, LANES), jnp.bfloat16),
            pltpu.VMEM((halves, share, stations, beams, LANES), jnp.bfloat16),
            pltpu.VMEM((share, stations, result_rows, LANES), jnp.float32),
            pltpu.VMEM((share, stations // 2, result_rows, LANES), jnp.bfloat16),
            pltpu.VMEM((share, stations // 2, result_rows, LANES), jnp.float32),
            pltpu.VMEM((share, stations // 2, result_rows, LANES), jnp.bfloat16),
            pltpu.VMEM((8, LANES), jnp.float32),
            pltpu.VMEM((groups - 1, 8, LANES), jnp.float32),
            dma((2,)),
            dma((CHUNKS_IN_FLIGHT,)),
            dma((groups - 1,)),
            dma((groups - 1,)),
            dma,
            dma((groups - 1, halves, share, quarters)),
            dma,
            dma((share,)),
            dma,
            dma,
            dma,
            dma,
        ],
        compiler_params=pltpu.CompilerParams(
            collective_id=0, has_side_effects=True, vmem_limit_bytes=56000000
        ),
    )(subband_table, antenna_flags, samples, slabs)
    return out.transpose(3, 0, 1, 2)[:, :, None]


def solution(mesh):
    in_specs = (
        P(None, "station", "chan", None, None),
        P(None, "station", None, "chan", None),
        P("station", "chan"),
        P(),
    )
    out_specs = P("chan", None, "station", None, None)
    return jax.shard_map(
        on_device, mesh=mesh, in_specs=in_specs, out_specs=out_specs, check_vma=False
    )
```

```python
import functools

import jax
import jax.numpy as jnp
from jax import lax
from jax.experimental import pallas as pl
from jax.experimental.pallas import tpu as pltpu
from jax.sharding import PartitionSpec as P

LANES = 128
SLAB = 64
SLABS_PER_CHUNK = 8
CHUNKS_IN_FLIGHT = 5
GROUP = 8
UNROLL = 16
TILE_BEAMS = 16
AHEAD = 3
BEHIND = 3


def split(value):
    high = value.astype(jnp.bfloat16)
    low = (value - high.astype(jnp.float32)).astype(jnp.bfloat16)
    return high, low


def kernel(
    table_hbm, flags_hbm, x_hbm, w_hbm, out_ref,
    table_ref, flags_ref, rows, chunk_buf, own, partials, arrived, gathered, results, far_results, returned, far_returned, count_ref, counts,
    small_sem, chunk_sem, count_send, count_recv, chan_send, chan_recv, beam_send, beam_recv, back_send, back_recv,
    far_send, far_recv,
):
    groups, stations = lax.axis_size("chan"), lax.axis_size("station")
    mine, me = lax.axis_index("chan"), lax.axis_index("station")
    halves, share = gathered.shape[0], gathered.shape[1]
    antennas = x_hbm.shape[2]
    subbands = x_hbm.shape[4]
    beams = gathered.shape[3]
    kept = subbands // groups
    blocks = subbands // LANES
    tall = min(antennas, SLAB)
    stride = rows.shape[1]
    w_first = halves * antennas
    w_chunks = w_hbm.shape[2] // SLABS_PER_CHUNK
    x_chunks = antennas // SLABS_PER_CHUNK
    chunks = w_chunks + halves * x_chunks
    beams_per_chunk = SLABS_PER_CHUNK * SLAB // antennas
    parts_of_phase = stations // GROUP
    lines = rows.reshape(subbands * stride, LANES)

    def target(k):
        middle = stations // 2
        side = me // middle
        across = (1 - side) * middle + lax.rem(me + k, middle)
        beside = side * middle + lax.rem(me + 1 + k, middle)
        return jnp.where(k < middle, across, beside)

    def remote(src, dst, send, recv, device):
        return pltpu.make_async_remote_copy(
            src_ref=src, dst_ref=dst, send_sem=send, recv_sem=recv,
            device_id=device, device_id_type=pl.DeviceIdType.MESH,
        )

    def chan_copy(g, h, i, q):
        peer = lax.rem(mine + g, groups)
        return remote(
            partials.at[g - 1, h, i, q], arrived.at[g - 1, h, i, q],
            chan_send, chan_recv.at[g - 1, h, i, q], (me, peer),
        )

    def count_copy(g):
        return remote(
            count_ref, counts.at[g - 1], count_send.at[g - 1], count_recv.at[g - 1], (me, lax.rem(mine + g, groups))
        )

    def beam_copy(h, i, q, u):
        return remote(
            arrived.at[0, h, i, q, u], gathered.at[h, i, me],
            beam_send, beam_recv.at[i], (target(q * GROUP + u), mine),
        )

    half = stations // 2
    near_first = me // half * half
    far_first = half - near_first

    def back_copy(i, k):
        there = near_first + lax.rem(me + 1 + k, half)
        return remote(
            results.at[i, there], returned.at[i, lax.rem(me, half)], back_send, back_recv, (there, mine)
        )

    def far_copy(i, k):
        return remote(
            far_results.at[i, k], far_returned.at[i, lax.rem(me, half)], far_send, far_recv,
            (far_first + k, mine),
        )

    def all_of(ref, send, recv):
        return remote(ref, ref, send, recv, (me, lax.rem(mine + 1, groups)))

    others = pl.ds(0, stations - 1)

    def w_copy(n, slot):
        return pltpu.make_async_copy(
            w_hbm.at[:, 0, pl.ds(n * SLABS_PER_CHUNK, SLABS_PER_CHUNK)], chunk_buf.at[slot], chunk_sem.at[slot]
        )

    def x_copy(n, slot):
        half = n // x_chunks
        first = lax.rem(n, x_chunks) * SLABS_PER_CHUNK
        return pltpu.make_async_copy(
            x_hbm.at[:, 0, pl.ds(first, SLABS_PER_CHUNK), pl.ds(half * SLAB, SLAB)],
            chunk_buf.at[slot], chunk_sem.at[slot],
        )

    def slot_of(n):
        return lax.rem(n, CHUNKS_IN_FLIGHT)

    def start_chunk(n):
        @pl.when(n < w_chunks)
        def _():
            w_copy(n, slot_of(n)).start()

        @pl.when((n >= w_chunks) & (n < chunks))
        def _():
            x_copy(n - w_chunks, slot_of(n)).start()

    flags_copy = pltpu.make_async_copy(flags_hbm, flags_ref, small_sem.at[0])
    table_copy = pltpu.make_async_copy(table_hbm, table_ref, small_sem.at[1])
    flags_copy.start()
    table_copy.start()
    for n in range(min(CHUNKS_IN_FLIGHT, chunks)):
        if n < w_chunks:
            w_copy(n, n % CHUNKS_IN_FLIGHT).start()
        else:
            x_copy(n - w_chunks, n % CHUNKS_IN_FLIGHT).start()

    barrier = pltpu.get_barrier_semaphore()
    for g in range(1, groups):
        pl.semaphore_signal(
            barrier, inc=1, device_id=(me, lax.rem(mine + g, groups)), device_id_type=pl.DeviceIdType.MESH
        )

    @pl.loop(0, stations - 1)
    def _(k):
        pl.semaphore_signal(barrier, inc=1, device_id=(target(k), mine), device_id_type=pl.DeviceIdType.MESH)

    flags_copy.wait()
    usable = flags_ref[...].astype(jnp.float32)
    count_ref[...] = jnp.broadcast_to(jnp.sum(usable, axis=1, keepdims=True), count_ref.shape)
    if antennas < LANES:
        usable = jnp.concatenate([usable, jnp.zeros((1, LANES - antennas), jnp.float32)], axis=1)

    @pl.loop(0, w_chunks)
    def _(n):
        slot = slot_of(n)
        w_copy(n, slot).wait()
        for part in range(2):
            for b in range(beams_per_chunk):
                for block in range(blocks):
                    lanes = slice(block * LANES, (block + 1) * LANES)
                    tiles = [
                        chunk_buf[slot, part, row // SLAB, row % SLAB : row % SLAB + tall, lanes]
                        for row in range(b * antennas, (b + 1) * antennas, tall)
                    ]
                    if antennas < LANES:
                        tiles.append(jnp.zeros((LANES - antennas, LANES), jnp.float32))
                    row = block * LANES * stride + w_first + part * beams + n * beams_per_chunk + b
                    lines[pl.ds(row, LANES, stride=stride), :] = jnp.concatenate(tiles, axis=0).T * usable
        start_chunk(n + CHUNKS_IN_FLIGHT)

    def turn(h, first, last):
        @pl.loop(first, last)
        def _(m):
            n = w_chunks + h * x_chunks + m
            slot = slot_of(n)
            x_copy(h * x_chunks + m, slot).wait()
            for a in range(SLABS_PER_CHUNK):
                for block in range(blocks):
                    lanes = pl.ds(block * LANES, LANES)
                    tile = jnp.concatenate([chunk_buf[slot, part, a, :, lanes] for part in range(2)], axis=0)
                    row = block * LANES * stride + h * antennas + m * SLABS_PER_CHUNK + a
                    lines[pl.ds(row, LANES, stride=stride), :] = tile.T
            start_chunk(n + CHUNKS_IN_FLIGHT)

    turn(0, 0, x_chunks)

    table_copy.wait()
    pl.semaphore_wait(barrier, groups - 1 + stations - 1)
    for g in range(1, groups):
        count_copy(g).start()

    lane = lax.broadcasted_iota(jnp.int32, (beams, LANES), 1)
    sign = jnp.where(lane < SLAB, -1.0, 1.0).astype(jnp.float32)

    def partial(h, slot):
        f = table_ref[slot]
        x = rows[f, pl.ds(pl.multiple_of(h * antennas, 8), antennas), :]
        w = rows[f, w_first : w_first + 2 * beams, :antennas]
        x_pair = jnp.concatenate(split(x), axis=0)
        w_high, w_low = split(w)
        grid = jnp.dot(
            jnp.concatenate([w_high, w_high], axis=1), x_pair, preferred_element_type=jnp.float32
        ) + jnp.dot(jnp.concatenate([w_low, w_low], axis=1), x_pair, preferred_element_type=jnp.float32)
        return grid[:beams] + pltpu.roll(grid[beams:], SLAB, axis=1) * sign

    def peers(h, i):
        for g in range(1, groups):
            first = lax.rem(mine + g, groups) * kept + i * stations

            @pl.loop(0, stations // UNROLL)
            def _(v):
                for w in range(UNROLL // GROUP):
                    q = v * (UNROLL // GROUP) + w
                    for u in range(GROUP):
                        total = partial(h, first + target(q * GROUP + u))
                        partials[g - 1, h, i, q, u] = total.astype(jnp.bfloat16)
                    chan_copy(g, h, i, q).start()

    def own_sums(h, i):
        first = mine * kept + i * stations

        @pl.loop(0, stations // UNROLL)
        def _(v):
            for w in range(UNROLL // GROUP):
                q = v * (UNROLL // GROUP) + w
                for u in range(GROUP):
                    own[q, u] = partial(h, first + target(q * GROUP + u))

    def forward(h, i, gain):
        def piece(q, last):
            for g in range(1, groups):
                chan_copy(g, h, i, q).wait_recv()
            for u in range(GROUP):
                total = own[q, u]
                for g in range(1, groups):
                    total = total + arrived[g - 1, h, i, q, u].astype(jnp.float32)
                value = (total * gain).astype(jnp.bfloat16)
                if last and u == GROUP - 1:
                    gathered[h, i, me] = value
                else:
                    arrived[0, h, i, q, u] = value
                    beam_copy(h, i, q, u).start()

        @pl.loop(0, parts_of_phase - 1)
        def _(q):
            piece(q, False)

        piece(parts_of_phase - 1, True)

    tile_rows = stations * TILE_BEAMS
    mask = lax.broadcasted_iota(jnp.int32, (TILE_BEAMS, tile_rows), 0) == lax.rem(
        lax.broadcasted_iota(jnp.int32, (TILE_BEAMS, tile_rows), 1), TILE_BEAMS
    )
    chosen = mask.astype(jnp.float32).reshape(1, TILE_BEAMS, tile_rows)
    wide = tile_rows // LANES
    beam_tiles = beams // TILE_BEAMS
    result_rows = 2 * beam_tiles * wide

    def spare(shape, station):
        row, place = lax.broadcasted_iota(jnp.int32, shape, 1), lax.broadcasted_iota(jnp.int32, shape, 2)
        other = lax.rem(row, wide) * (LANES // TILE_BEAMS) + place // TILE_BEAMS
        return (row >= result_rows // 2) & (other == station)

    def correlate(i):
        all_of(gathered.at[:, i, others], beam_send, beam_recv.at[i]).wait_recv()
        for tile in range(beam_tiles):
            straight, turned = [], []
            for h in range(halves):
                y = gathered[h, i, :, pl.ds(tile * TILE_BEAMS, TILE_BEAMS), :].reshape(tile_rows, LANES)
                straight.append(y)
                swapped = jnp.concatenate([y[:, SLAB:], -y[:, :SLAB]], axis=1)
                turned.append(swapped)
            y = jnp.concatenate(straight, axis=1)
            for part, x in enumerate((y, jnp.concatenate(turned, axis=1))):
                pairs = lax.dot_general(x, y, (((1,), (1,)), ((), ())), preferred_element_type=jnp.float32)
                total = jnp.sum(pairs.reshape(stations, TILE_BEAMS, tile_rows) * chosen, axis=1)
                for piece in range(wide):
                    row = (part * beam_tiles + tile) * wide + piece
                    results[i, :, row, :] = total[:, piece * LANES : (piece + 1) * LANES]

        value = results[i, pl.ds(far_first, half)]
        low = value - value.astype(jnp.bfloat16).astype(jnp.float32)
        station = far_first + lax.broadcasted_iota(jnp.int32, value.shape, 0)
        far_results[i] = jnp.where(
            spare(value.shape, station), pltpu.roll(low, result_rows // 2, axis=1), value
        ).astype(jnp.bfloat16)

        @pl.loop(0, half)
        def _(k):
            far_copy(i, k).start()

        @pl.loop(0, half - 1)
        def _(k):
            back_copy(i, k).start()

        returned[i, lax.rem(me, half)] = results[i, me]

    phases = halves * share
    ahead, behind = min(AHEAD, share), min(BEHIND, share)
    each = pl.cdiv(x_chunks, share - ahead + 1)

    for p in range(ahead):
        peers(0, p)
    count = count_ref[...]
    for g in range(1, groups):
        count_copy(g).wait_recv()
        count = count + counts[g - 1]
    gain = lax.rsqrt(count)[0:1, :]

    @pl.loop(0, phases)
    def _(p):
        own_sums(p // share, lax.rem(p, share))
        forward(p // share, lax.rem(p, share), gain)

        turn(1, jnp.minimum(p * each, x_chunks * (halves - 1)), jnp.minimum((p + 1) * each, x_chunks * (halves - 1)))

        @pl.when(p + ahead < phases)
        def _():
            peers((p + ahead) // share, lax.rem(p + ahead, share))

        @pl.when(p >= phases - share + behind)
        def _():
            correlate(p - (phases - share + behind))

    @pl.loop(share - behind, share)
    def _(i):
        correlate(i)

    all_of(returned.at[:, pl.ds(0, half - 1)], back_send, back_recv).wait_recv()
    all_of(results.at[:, pl.ds(0, half - 1)], back_send, back_recv).wait_send()
    all_of(far_returned, far_send, far_recv).wait_recv()
    for i in range(share):
        value = far_returned[i].astype(jnp.float32)
        extra = spare(value.shape, me)
        low = pltpu.roll(jnp.where(extra, value, 0.0), result_rows // 2, axis=1)
        results[i, pl.ds(far_first, half)] = jnp.where(extra, 0.0, value + low)
        results[i, pl.ds(near_first, half)] = returned[i]

    per_row = LANES // TILE_BEAMS
    for part in range(2):
        for tile in range(beam_tiles):
            for piece in range(wide):
                row = (part * beam_tiles + tile) * wide + piece
                turned = results[:, :, row, :].reshape(kept, LANES).T
                for r in range(per_row):
                    out_ref[part, pl.ds(tile * TILE_BEAMS, TILE_BEAMS), piece * per_row + r, :] = turned[
                        r * TILE_BEAMS : (r + 1) * TILE_BEAMS
                    ]

    for g in range(1, groups):
        count_copy(g).wait_send()
    all_of(partials, chan_send, chan_recv.at[0, 0, 0, 0]).wait_send()
    all_of(gathered.at[:, :, others], beam_send, beam_recv.at[0]).wait_send()
    all_of(far_results, far_send, far_recv).wait_send()


def on_device(samples, weights, antenna_flags, subband_table):
    groups, stations = lax.axis_size("chan"), lax.axis_size("station")
    _, _, antennas, times, subbands = samples.shape
    beams = weights.shape[2]
    kept = subbands // groups
    share = kept // stations
    halves = times // SLAB
    quarters = stations // GROUP
    result_rows = 2 * (beams // TILE_BEAMS) * (stations * TILE_BEAMS // LANES)
    slabs = weights.reshape(2, 1, beams * antennas // SLAB, SLAB, subbands)
    dma = pltpu.SemaphoreType.DMA
    out = pl.pallas_call(
        kernel,
        out_shape=jax.ShapeDtypeStruct((2, beams, stations, kept), jnp.float32),
        in_specs=[
            pl.BlockSpec(memory_space=pltpu.HBM),
            pl.BlockSpec(memory_space=pltpu.HBM),
            pl.BlockSpec(memory_space=pl.ANY),
            pl.BlockSpec(memory_space=pl.ANY),
        ],
        out_specs=pl.BlockSpec(memory_space=pltpu.VMEM),
        scratch_shapes=[
            pltpu.SMEM((subbands,), jnp.int32),
            pltpu.VMEM((1, antennas), jnp.int32),
            pltpu.VMEM((subbands, halves * antennas + 2 * beams + 8, LANES), jnp.float32),
            pltpu.VMEM((CHUNKS_IN_FLIGHT, 2, SLABS_PER_CHUNK, SLAB, subbands), jnp.float32),
            pltpu.VMEM((quarters, GROUP, beams, LANES), jnp.float32),
            pltpu.VMEM((groups - 1, halves, share, quarters, GROUP, beams, LANES), jnp.bfloat16),
            pltpu.VMEM((groups - 1, halves, share, quarters, GROUP, beams, LANES), jnp.bfloat16),
            pltpu.VMEM((halves, share, stations, beams, LANES), jnp.bfloat16),
            pltpu.VMEM((share, stations, result_rows, LANES), jnp.float32),
            pltpu.VMEM((share, stations // 2, result_rows, LANES), jnp.bfloat16),
            pltpu.VMEM((share, stations // 2, result_rows, LANES), jnp.float32),
            pltpu.VMEM((share, stations // 2, result_rows, LANES), jnp.bfloat16),
            pltpu.VMEM((8, LANES), jnp.float32),
            pltpu.VMEM((groups - 1, 8, LANES), jnp.float32),
            dma((2,)),
            dma((CHUNKS_IN_FLIGHT,)),
            dma((groups - 1,)),
            dma((groups - 1,)),
            dma,
            dma((groups - 1, halves, share, quarters)),
            dma,
            dma((share,)),
            dma,
            dma,
            dma,
            dma,
        ],
        compiler_params=pltpu.CompilerParams(
            collective_id=0, has_side_effects=True, vmem_limit_bytes=56000000
        ),
    )(subband_table, antenna_flags, samples, slabs)
    return out.transpose(3, 0, 1, 2)[:, :, None]


def solution(mesh):
    in_specs = (
        P(None, "station", "chan", None, None),
        P(None, "station", None, "chan", None),
        P("station", "chan"),
        P(),
    )
    out_specs = P("chan", None, "station", None, None)
    return jax.shard_map(
        on_device, mesh=mesh, in_specs=in_specs, out_specs=out_specs, check_vma=False
    )
```
